512 devices in a mesh: group: 2 (over y), dev: 128 (over x, z), tp: 2 (over core).
Axes of the slice: x: 8, y: 2, z: 16, core: 2. Of those that a mesh axis runs over, the one named last changes fastest.
The devices are a block of a 8x8x16 slice.
Arguments:
- prompt_activations: bfloat16 [65536, 8192], P(('group', 'dev')), parts along dimension 0, may hold values from -6 to 6
- key_matrix: bfloat16 [8192, 512], P('dev', 'tp'), may hold values from -0.0625 to 0.0625
- value_matrix: bfloat16 [8192, 512], P('dev', 'tp'), may hold values from -0.0625 to 0.0625
- adapter_down_keyvalue: bfloat16 [8192, 128], P('dev'), may hold values from -0.0625 to 0.0625
- adapter_up_key: bfloat16 [64, 512], P(None, 'tp'), may hold values from -1.5 to 1.5
- adapter_up_value: bfloat16 [64, 512], P(None, 'tp'), may hold values from -1.5 to 1.5
- request_adapter: int32 [256], P('group'), parts along dimension 0, may hold values from 0 to 3
- page_request: int32 [16384, 1], P('group'), parts along dimension 0, may hold values from 0 to 127; in each aligned block of 64 rows (0 to 63, 64 to 127, ...) at most 2 rows name the same one
- context_tokens: int32 [256], P('group'), parts along dimension 0, may hold values from 64 to 256
- step_query: bfloat16 [256, 4096], P(('group', 'dev'), 'tp'), parts along dimension 0, may hold values from -256 to 256
- step_key: bfloat16 [256, 512], P(('group', 'dev'), 'tp'), parts along dimension 0, may hold values from -6 to 6
- step_value: bfloat16 [256, 512], P(('group', 'dev'), 'tp'), parts along dimension 0, may hold values from -6 to 6
- stored_keys: bfloat16 [256, 256, 512], P(('group', 'dev'), None, 'tp'), parts along dimension 0, may hold values from -6 to 6
- stored_values: bfloat16 [256, 256, 512], P(('group', 'dev'), None, 'tp'), parts along dimension 0, may hold values from -6 to 6
- output_matrix: bfloat16 [4096, 8192], P('tp', 'dev'), may hold values from -0.09375 to 0.09375
- adapter_down_output: bfloat16 [4096, 64], P('tp'), may hold values from -0.09375 to 0.09375
- adapter_up_output: bfloat16 [64, 8192], P(None, 'dev'), may hold values from -1.5 to 1.5
Outputs:
- attended: bfloat16 [256, 8192], P('group', 'dev'), parts along dimension 0
The draws below stay inside these ranges and needn't reach their ends.
There are 2 independent parts, one for each index of `group`. The reference program is written for one: setup_inputs(seed, part) draws one part's arguments, and reference() takes and returns one part's arrays. A program takes and returns all parts, laid end to end along the dimension named above; an argument that names none is the same for every part. Nothing has to cross between parts.
Inputs may be any that keep to these rules, and one draw needn't show every extreme that they name: `page_request`: among the pages of one device's prompt block (aligned blocks of 64 pages), no request owns more than 2; every request owns at least one page.
All inputs are finite; a program needn't handle non-finite values.
Results may differ from the reference program's by a relative error of at most 0.0086.
Values may be sent and summed in bfloat16 or wider, within the bound.
No kernel may reach another device: no remote copies, remote signals or barrier semaphores. Data moves between devices by JAX's collectives and lax.ppermute only.
A program may use at most 64 MiB of HBM per device.

```python
import math
import jax
import jax.numpy as jnp
import numpy as np
from jax import lax

MODEL_WIDTH = 8192
HEADS = 32
KV_HEADS = 4
HEAD = 128
LOW_RANK = 16
ADAPTER_COUNT = 4
TOK_DEV = 256
PAGE = 4
CTX = 256
CAP = 2
QUERY_WIDTH = 4096
KEY_WIDTH = 512
ROWS = 128
TOKENS = 32768
PAGES = 8192
N_DEV = 128


def drawn_draw(key):
    base_key = jax.random.fold_in(jax.random.fold_in(key, 7), 3)
    base_keys = jnp.clip(jax.random.normal(base_key, (ROWS, CTX, KEY_WIDTH), jnp.float32), -6.0, 6.0)
    return base_keys


def draw_stored_keys(key, part):
    base_keys = drawn_draw(key)
    return base_keys.astype(jnp.bfloat16)


def draw_step_query(key, part):
    normal_part = jnp.clip(2.0 * jax.random.normal(jax.random.fold_in(key, 11), (ROWS, QUERY_WIDTH), jnp.float32), -12.0, 12.0)
    return normal_part.astype(jnp.bfloat16)


def with_ends(array, key, smallest, top_value):
    spot = [jax.random.randint(jax.random.fold_in(key, axis), (), 0, length) for axis, length in enumerate(array.shape)]
    longest = array.shape.index(max(array.shape))
    neighbour = spot[:longest] + [(spot[longest] + 1) % array.shape[longest]] + spot[longest + 1:]
    return array.at[tuple(spot)].set(smallest).at[tuple(neighbour)].set(top_value)


def block_levels(own_key, dims, cuts, low, largest):
    level, own = 1.0, jax.random.fold_in(own_key, 6)
    for axis_at, parts in cuts:
        draws = jnp.exp(jax.random.uniform(jax.random.fold_in(own, axis_at), (parts,), jnp.float32, low / len(cuts), largest / len(cuts)))
        level = level * jnp.repeat(draws, dims[axis_at] // parts).reshape([-1 if axis == axis_at else 1 for axis in range(len(dims))])
    return level


def assign_block(key, own, number, rows, amount, top, bound, skew):
    order = jax.random.permutation(key, amount)
    heavy_load, usual = portions_of(amount, rows * top, bound, skew, True), portions_of(amount, rows * top, bound, skew, False)
    places = jnp.arange(amount)

    def named(tallies, offset_by):
        used = int((tallies > 0).sum())
        fixed = max(1, used // 4)
        passed = fixed + (places - fixed + offset_by * (used - fixed)) % max(1, amount - fixed)
        return jnp.zeros((amount,), jnp.int32).at[order[jnp.where(places < fixed, places, passed)]].set(jnp.asarray(tallies, jnp.int32))

    tallies = jnp.where(number % 4 == 0, named(heavy_load, number // 4), named(usual, number - number // 4 - 1))
    mixed = jax.random.permutation(jax.random.fold_in(own, 3), amount)
    donor, receiver = mixed[0:amount // 2 * 2:2], mixed[1:amount // 2 * 2:2]
    room = jnp.minimum(tallies[donor] - 1, bound - tallies[receiver]) // 2
    room = jnp.where((donor == order[0]) | (receiver == order[0]) | (tallies[receiver] == 0), 0, jnp.maximum(room, 0))
    passed = jax.random.randint(jax.random.fold_in(own, 4), (amount // 2,), 0, 1 << 20) % (room + 1)
    tallies = tallies.at[donor].add(-passed).at[receiver].add(passed)
    members = jnp.searchsorted(jnp.cumsum(tallies), jnp.arange(rows * top), side="right").astype(jnp.int32)
    grid = members.reshape(top, rows).T
    grid = grid[jax.random.permutation(jax.random.fold_in(own, 1), rows)]
    offset_by = jax.random.randint(jax.random.fold_in(own, 2), (rows, 1), 0, top)
    return jnp.take_along_axis(grid, (jnp.arange(top)[None, :] + offset_by) % top, axis=1)


def portions_of(count, total, bound, lean, full):
    loads = [(1 << 20) // math.isqrt(standing ** lean) + 1 for standing in range(1, count + 1)]
    largest = bound if full else min(bound, max(-(-total // count), total * loads[0] // sum(loads)))
    least = 1 if total - largest >= count - 1 else 0
    given, spare = [largest] + [least] * (count - 1), total - largest - least * (count - 1)
    while spare > 0:
        candidates = [i for i in range(1, count) if given[i] < largest] or [i for i in range(1, count) if given[i] < bound]
        pool, remaining = sum([loads[i] for i in candidates]), spare
        for i in candidates:
            more = min(bound - given[i], max(1, remaining * loads[i] // pool), spare)
            given[i] = given[i] + more
            spare = spare - more
    return np.array(given)


def normal_values(rng, dims, scale, most, shards=(), kind=jnp.bfloat16):
    level = block_levels(rng, dims, shards, -0.22, 0.18) if shards else 1.0
    result = jax.random.normal(rng, dims, jnp.float32) * scale * level
    return jnp.minimum(jnp.maximum(result, -most), most).astype(kind)


def setup_inputs(seed: int = 0, part: int = 0) -> dict:
    splits = jax.random.split(jax.random.key(seed), 18)
    own_keys = jax.random.split(jax.random.fold_in(splits[17], part), 18)
    prompt_activations = normal_values(own_keys[0], (TOKENS, MODEL_WIDTH), 1.0, 6.0, ((0, 128),))
    key_matrix = normal_values(splits[1], (MODEL_WIDTH, KEY_WIDTH), MODEL_WIDTH ** -0.5, 0.0625, ((0, 128), (1, 2)))
    value_matrix = normal_values(splits[2], (MODEL_WIDTH, KEY_WIDTH), MODEL_WIDTH ** -0.5, 0.0625, ((0, 128), (1, 2)))
    adapter_down_keyvalue = normal_values(splits[3], (MODEL_WIDTH, 2 * ADAPTER_COUNT * LOW_RANK), MODEL_WIDTH ** -0.5, 0.0625, ((0, 128),))
    adapter_up_key = normal_values(splits[4], (ADAPTER_COUNT * LOW_RANK, KEY_WIDTH), LOW_RANK ** -0.5, 1.5, ((1, 2),))
    adapter_up_value = normal_values(splits[5], (ADAPTER_COUNT * LOW_RANK, KEY_WIDTH), LOW_RANK ** -0.5, 1.5, ((1, 2),))
    request_adapter = with_ends(jax.random.randint(own_keys[6], (ROWS,), 0, ADAPTER_COUNT), jax.random.fold_in(own_keys[6], 1), 0, ADAPTER_COUNT - 1).astype(jnp.int32)
    page_request_keys = jax.random.split(jax.random.fold_in(own_keys[7], 1), PAGES // (TOK_DEV // PAGE))
    page_request_turns = jax.random.permutation(jax.random.fold_in(own_keys[7], 3), PAGES // (TOK_DEV // PAGE))
    page_request = jax.vmap(lambda own, number: assign_block(jax.random.fold_in(own_keys[7], 2), own, number, TOK_DEV // PAGE, ROWS, 1, CAP, 2))(page_request_keys, page_request_turns).reshape((PAGES, 1))
    context_tokens = with_ends(jax.random.randint(own_keys[8], (ROWS,), CTX // 4, CTX + 1), jax.random.fold_in(own_keys[8], 1), CTX // 4, CTX).astype(jnp.int32)
    step_query = draw_step_query(jax.random.fold_in(jax.random.fold_in(splits[17], part), 71), part)
    step_key = normal_values(own_keys[10], (ROWS, KEY_WIDTH), 1.0, 6.0, ((0, 128), (1, 2)))
    step_value = normal_values(own_keys[11], (ROWS, KEY_WIDTH), 1.0, 6.0, ((0, 128), (1, 2)))
    stored_keys = draw_stored_keys(jax.random.fold_in(jax.random.fold_in(splits[17], part), 71), part)
    stored_values = normal_values(own_keys[13], (ROWS, CTX, KEY_WIDTH), 1.0, 6.0, ((0, 128), (2, 2)))
    output_matrix = normal_values(splits[14], (QUERY_WIDTH, MODEL_WIDTH), QUERY_WIDTH ** -0.5, 0.09375, ((0, 2), (1, 128)))
    adapter_down_output = normal_values(splits[15], (QUERY_WIDTH, ADAPTER_COUNT * LOW_RANK), QUERY_WIDTH ** -0.5, 0.09375, ((0, 2),))
    adapter_up_output = normal_values(splits[16], (ADAPTER_COUNT * LOW_RANK, MODEL_WIDTH), LOW_RANK ** -0.5, 1.5, ((1, 128),))
    return dict(prompt_activations=prompt_activations, key_matrix=key_matrix, value_matrix=value_matrix, adapter_down_keyvalue=adapter_down_keyvalue, adapter_up_key=adapter_up_key, adapter_up_value=adapter_up_value, request_adapter=request_adapter, page_request=page_request, context_tokens=context_tokens, step_query=step_query, step_key=step_key, step_value=step_value, stored_keys=stored_keys, stored_values=stored_values, output_matrix=output_matrix, adapter_down_output=adapter_down_output, adapter_up_output=adapter_up_output)


adapter_scale = 1.0
rope_base = 500000.0


def rotate(key_rows, positions):
    row_count = key_rows.shape[0]
    blocks = key_rows.reshape(row_count, -1, HEAD)
    half_size = HEAD // 2
    exponent = jnp.arange(half_size, dtype=jnp.float32) * (2.0 / HEAD)
    frequency = jnp.exp(-jnp.log(jnp.float32(rope_base)) * exponent)
    angles = positions.astype(jnp.float32)[:, None] * frequency[None, :]
    cosine = jnp.cos(angles)[:, None, :]
    sine_part = jnp.sin(angles)[:, None, :]
    first_half = blocks[..., :half_size]
    second_half = blocks[..., half_size:]
    turned = jnp.concatenate([first_half * cosine - second_half * sine_part, second_half * cosine + first_half * sine_part], axis=-1)
    return turned.reshape(row_count, -1)


def owner_ranks(owners, row_total):
    onehot = (owners[:, None] == jnp.arange(row_total, dtype=jnp.int32)[None, :]).astype(jnp.int32)
    before = jnp.cumsum(onehot, axis=0) - onehot
    rank = jnp.sum(before * onehot, axis=1).astype(jnp.int32)
    return onehot, rank


def mask_columns(narrowed, adapter_list):
    column = jnp.arange(narrowed.shape[1], dtype=jnp.int32)
    owner = (column % (ADAPTER_COUNT * LOW_RANK)) // LOW_RANK
    return jnp.where(owner[None, :] == adapter_list[:, None], narrowed, jnp.zeros_like(narrowed))


def selected_narrow(activation_rows, adapter_down, adapter_list):
    narrowed = jnp.dot(activation_rows, adapter_down, preferred_element_type=jnp.float32)
    return mask_columns(narrowed, adapter_list)


def widened(selected_rows, up_key, up_value):
    split_at = ADAPTER_COUNT * LOW_RANK
    highest = lax.Precision.HIGHEST
    key_portion = jnp.dot(selected_rows[:, :split_at], up_key.astype(jnp.float32), precision=highest)
    value_portion = jnp.dot(selected_rows[:, split_at:], up_value.astype(jnp.float32), precision=highest)
    return adapter_scale * key_portion, adapter_scale * value_portion


def attend(query, old_keys, old_values, old_length, fresh_keys, fresh_values, fresh_valid, last_key, last_value):
    all_keys = jnp.concatenate([old_keys, fresh_keys, last_key[None, :]], axis=0).astype(jnp.float32)
    all_values = jnp.concatenate([old_values, fresh_values, last_value[None, :]], axis=0).astype(jnp.float32)
    old_valid = jnp.arange(old_keys.shape[0], dtype=jnp.int32) < old_length
    valid = jnp.concatenate([old_valid, fresh_valid, jnp.ones((1,), dtype=bool)])
    group_size = HEADS // KV_HEADS
    query_heads = query.astype(jnp.float32).reshape(-1, group_size, HEAD)
    key_count = all_keys.shape[0]
    key_heads = all_keys.reshape(key_count, -1, HEAD)
    value_heads = all_values.reshape(key_count, -1, HEAD)
    scores = jnp.einsum("kgd,lkd->kgl", query_heads, key_heads) * (HEAD ** -0.5)
    scores = jnp.where(valid[None, None, :], scores, -1e30)
    top = jnp.max(scores, axis=-1, keepdims=True)
    weights = jnp.exp(scores - top)
    total = jnp.sum(weights, axis=-1, keepdims=True)
    probs = (weights / total).astype(jnp.bfloat16)
    output = jnp.einsum("kgl,lkd->kgd", probs.astype(jnp.float32), value_heads)
    return output.reshape(-1).astype(jnp.bfloat16)


def reference(prompt_activations, key_matrix, value_matrix, adapter_down_keyvalue, adapter_up_key, adapter_up_value, request_adapter, page_request, context_tokens, step_query, step_key, step_value, stored_keys, stored_values, output_matrix, adapter_down_output, adapter_up_output):
    token_total = prompt_activations.shape[0]
    owners = page_request[:, 0].astype(jnp.int32)
    pages_total = owners.shape[0]
    onehot, rank = owner_ranks(owners, ROWS)
    tokens = jnp.arange(token_total, dtype=jnp.int32)
    token_page = tokens // PAGE
    token_row = jnp.take(owners, token_page)
    position = (jnp.take(context_tokens, token_row) + jnp.take(rank, token_page) * PAGE + tokens % PAGE).astype(jnp.int32)
    adapter_list = jnp.take(request_adapter, token_row).astype(jnp.int32)
    selected_rows = selected_narrow(prompt_activations, adapter_down_keyvalue, adapter_list)
    key_delta, value_delta = widened(selected_rows, adapter_up_key, adapter_up_value)
    key_raw = jnp.dot(prompt_activations, key_matrix, preferred_element_type=jnp.float32) + key_delta
    value_raw = jnp.dot(prompt_activations, value_matrix, preferred_element_type=jnp.float32) + value_delta
    new_keys = rotate(key_raw, position).astype(jnp.bfloat16)
    new_values = value_raw.astype(jnp.bfloat16)
    list_width = N_DEV * CAP
    table = jnp.zeros((ROWS * list_width,), jnp.int32).at[owners * list_width + rank].set(jnp.arange(pages_total, dtype=jnp.int32))
    counts = jnp.sum(onehot, axis=0).astype(jnp.int32)
    slot = jnp.arange(list_width * PAGE, dtype=jnp.int32)

    def attend_row(row):
        page_list = lax.dynamic_slice_in_dim(table, (row * list_width).astype(jnp.int32), list_width, 0)
        token_index = (jnp.take(page_list, slot // PAGE) * PAGE + slot % PAGE).astype(jnp.int32)
        fresh_keys = jnp.take(new_keys, token_index, axis=0)
        fresh_values = jnp.take(new_values, token_index, axis=0)
        fresh_valid = slot < jnp.take(counts, row) * PAGE
        return attend(step_query[row], stored_keys[row], stored_values[row], jnp.take(context_tokens, row), fresh_keys, fresh_values, fresh_valid, step_key[row], step_value[row])

    blended = lax.map(attend_row, jnp.arange(ROWS, dtype=jnp.int32))
    plain_result = jnp.dot(blended, output_matrix, preferred_element_type=jnp.float32)
    selected_output = selected_narrow(blended, adapter_down_output, request_adapter)
    adapter_delta = adapter_scale * jnp.dot(selected_output, adapter_up_output.astype(jnp.float32), precision=lax.Precision.HIGHEST)
    return (plain_result + adapter_delta).astype(jnp.bfloat16)
```

```python
import functools

import jax
import jax.numpy as jnp
from jax import lax
from jax.experimental import pallas as pl
from jax.experimental.pallas import tpu as pltpu
from jax.sharding import Mesh
from jax.sharding import PartitionSpec as P

HEADS = 32
KV_HEADS = 4
HEAD = 128
LOW_RANK = 16
ADAPTER_COUNT = 4
PAGE = 4
LORA = ADAPTER_COUNT * LOW_RANK
DEV = ("x", "zh", "zm", "zp")
GROUP_DEV = ("group", "x", "zh", "zm", "zp")
Z8 = ("zh", "zm")
NEAR = ("x", "zm", "zp")
NX, NZH, NZM, NZP = 8, 4, 2, 2
NEG = -1e30

rope_base = 500000.0


f32 = jnp.float32
bf16 = jnp.bfloat16
SMEM = pl.BlockSpec(memory_space=pltpu.SMEM)
VMEM = pl.BlockSpec(memory_space=pltpu.VMEM)


def ring_x(x, step):
    return lax.ppermute(x, "x", [(i, (i + step) % NX) for i in range(NX)])


def swap_pair(x):
    return lax.ppermute(x, "zp", [(0, 1), (1, 0)])


def spread(x, axes, count):
    copies = jnp.broadcast_to(x[None], (count, *x.shape))
    return lax.all_to_all(copies, axes, 0, 0, tiled=True)


def split_kernel(p_ref, a_ref, mine_ref, other_ref):
    parity = p_ref[0]
    half = HEAD // 2
    lane = lax.broadcasted_iota(jnp.int32, (a_ref.shape[0], HEAD), 1)
    low = lane < half
    first = parity == 0
    for k in range(mine_ref.shape[1] // HEAD):
        t0 = a_ref[:, 2 * k * HEAD : (2 * k + 1) * HEAD].astype(f32)
        t1 = a_ref[:, (2 * k + 1) * HEAD : (2 * k + 2) * HEAD].astype(f32)
        even = jnp.where(low, t0, pltpu.roll(t1, half, 1))
        odd = jnp.where(low, pltpu.roll(t0, half, 1), t1)
        cols = slice(k * HEAD, (k + 1) * HEAD)
        mine_ref[:, cols] = jnp.where(first, even, odd).astype(bf16)
        other_ref[:, cols] = jnp.where(first, odd, even).astype(bf16)


def split_columns(act, parity):
    rows, width = act.shape
    block = 64
    out = jax.ShapeDtypeStruct((rows, width // 2), bf16)
    return pl.pallas_call(
        split_kernel,
        grid=(rows // block,),
        in_specs=[SMEM, pl.BlockSpec((block, width), lambda i: (i, 0))],
        out_specs=[pl.BlockSpec((block, width // 2), lambda i: (i, 0))] * 2,
        out_shape=[out, out],
        name="split_columns",
    )(parity, act)


def project_kernel(offsets, chunks, depth, x_ref, a_ref, *refs):
    out_ref = refs[-1]
    me = x_ref[0]
    total = jnp.zeros(out_ref.shape, f32)
    for i, off in enumerate(offsets):
        where = lax.rem(me + off, NX)
        for c in range(chunks):
            start = pl.multiple_of((where * chunks + c) * depth, depth)
            a = a_ref[:, pl.ds(start, depth)]
            w = refs[i * chunks + c][0:depth, :]
            total = total + jnp.dot(a, w, preferred_element_type=f32)
    out_ref[...] = total.astype(out_ref.dtype)


def project(act, offsets, pieces, depth, me, dtype):
    chunks = len(pieces) // len(offsets)
    width = pieces[0].shape[1]
    return pl.pallas_call(
        functools.partial(project_kernel, offsets, chunks, depth),
        in_specs=[SMEM] + [VMEM] * (1 + len(pieces)),
        out_specs=VMEM,
        out_shape=jax.ShapeDtypeStruct((act.shape[0], width), dtype),
        name="project",
    )(me, act, *pieces)


def two_terms(v):
    hi = v.astype(bf16)
    return hi, (v - hi.astype(f32)).astype(bf16)


def dot_fine(v, w):
    hi, lo = two_terms(v)
    return jnp.dot(hi, w, preferred_element_type=f32) + jnp.dot(lo, w, preferred_element_type=f32)


def three_terms(v):
    hi = v.astype(bf16).astype(f32)
    mid = (v - hi).astype(bf16).astype(f32)
    return hi, mid, v - hi - mid


def partial_kernel(
    heads, kv, s_ref, base_ref, other_ref, upk_ref, upv_ref, cos_ref, sin_ref,
    adapter_ref, owner_ref, q0_ref, q1_ref, out_ref,
):
    me, parity = s_ref[0], s_ref[1]
    tokens = base_ref.shape[0]
    rows = out_ref.shape[0]
    width = kv * HEAD
    raw = base_ref[...] + other_ref[...].astype(f32)
    column = lax.broadcasted_iota(jnp.int32, (tokens, 2 * LORA), 1)
    kept = lax.rem(column, LORA) // LOW_RANK == adapter_ref[...]
    chosen = jnp.where(kept, raw[:, 2 * width :], 0.0)
    key = raw[:, :width] + dot_fine(chosen[:, :LORA], upk_ref[...])
    value = (raw[:, width : 2 * width] + dot_fine(chosen[:, LORA:], upv_ref[...])).astype(bf16)
    turned = []
    for k in range(kv):
        part = key[:, k * HEAD : (k + 1) * HEAD]
        spun = part * cos_ref[...] + pltpu.roll(part, HEAD // 2, 1) * sin_ref[...]
        turned.append(spun.astype(bf16))
    source = q0_ref.shape[0]
    blocks = 4
    i = lax.broadcasted_iota(jnp.int32, (rows, source), 1)
    dest = lax.broadcasted_iota(jnp.int32, (rows, source), 0)
    block = lax.rem(i, blocks)
    z8 = lax.rem(i // blocks, NZH * NZM)
    off = i // (blocks * NZH * NZM)
    xs = lax.rem(off + me, NX)
    spot = xs * (NZM * NZP * NZH) + lax.rem(z8, NZM) * (NZP * NZH) + z8 // NZM
    hit0 = dest == spot + parity * NZH
    hit1 = dest == spot + (1 - parity) * NZH
    queries = []
    for b in range(blocks):
        pick0 = jnp.where(hit0 & (block == b), 1.0, 0.0).astype(bf16)
        pick1 = jnp.where(hit1 & (block == b), 1.0, 0.0).astype(bf16)
        got = jnp.dot(pick0, q0_ref[...], preferred_element_type=f32) + jnp.dot(
            pick1, q1_ref[...], preferred_element_type=f32
        )
        queries.append(got.astype(bf16))
    mask = lax.broadcasted_iota(jnp.int32, (rows, tokens), 0) == owner_ref[...]
    lane = lax.broadcasted_iota(jnp.int32, (rows, HEAD), 1)
    stat = jnp.zeros((rows, HEAD), f32)
    per_block = heads // blocks
    for h in range(heads):
        k = h // (heads // kv)
        at = (h % per_block) * HEAD
        q = queries[h // per_block][:, at : at + HEAD]
        s = lax.dot_general(q, turned[k], (((1,), (1,)), ((), ())), preferred_element_type=f32)
        s = jnp.where(mask, s * (HEAD ** (-0.5)), NEG)
        top = jnp.max(s, axis=1, keepdims=True)
        e = jnp.where(mask, jnp.exp(s - top), 0.0)
        total = jnp.sum(e, axis=1, keepdims=True)
        o = jnp.dot(
            e.astype(bf16), value[:, k * HEAD : (k + 1) * HEAD], preferred_element_type=f32
        )
        full = total > 0.0
        o = o * jnp.where(full, 1.0 / jnp.maximum(total, 1e-30), 0.0)
        out_ref[:, h * HEAD : (h + 1) * HEAD] = o.astype(bf16)
        lse = jnp.where(full, top + jnp.log(jnp.maximum(total, 1e-30)), NEG)
        hi, mid, lo = three_terms(lse)
        stat = jnp.where(lane == h, hi, stat)
        stat = jnp.where(lane == heads + h, mid, stat)
        stat = jnp.where(lane == 2 * heads + h, lo, stat)
    out_ref[:, heads * HEAD :] = stat.astype(bf16)


def reduce_rows(v, op):
    while v.shape[0] > 8:
        half = v.shape[0] // 2
        v = op(v[:half], v[half:])
    return op(v, pltpu.roll(v, NZH, 0))


def merge(heads, x_ref, zh, cache_o, cache_lse, out_ref, with_stat):
    rows = x_ref.shape[0]
    st = x_ref[:, heads * HEAD :].astype(f32)
    lse = st + pltpu.roll(st, HEAD - heads, 1) + pltpu.roll(st, HEAD - 2 * heads, 1)
    lane = lax.broadcasted_iota(jnp.int32, (rows, HEAD), 1)
    lse = jnp.where(lane < heads, lse, 0.0)
    top = reduce_rows(lse, jnp.maximum)
    if cache_o is not None:
        row = lax.rem(lax.broadcasted_iota(jnp.int32, (8, HEAD), 0), NZH)
        here = row == zh
        top = jnp.where(here, jnp.maximum(top, cache_lse), top)
        cache_w = jnp.where(here, jnp.exp(cache_lse - top), 0.0)
    w = jnp.exp(lse - jnp.tile(top, (rows // 8, 1)))
    total = reduce_rows(w, jnp.add)
    if cache_o is not None:
        total = total + cache_w
    for h in range(heads):
        cols = slice(h * HEAD, (h + 1) * HEAD)
        o = reduce_rows(w[:, h : h + 1] * x_ref[:, cols].astype(f32), jnp.add)
        if cache_o is not None:
            o = o + cache_w[:, h : h + 1] * cache_o[:, cols]
        out_ref[:, cols] = (o / total[:, h : h + 1]).astype(bf16)
    if with_stat:
        final = top + jnp.log(total)
        hi, mid, lo = three_terms(jnp.where(lane[:8] < heads, final, 0.0))
        stat = hi + pltpu.roll(mid, heads, 1) + pltpu.roll(lo, 2 * heads, 1)
        out_ref[:, heads * HEAD :] = stat.astype(bf16)


def merge_first_kernel(heads, s_ref, x_ref, o_ref, lse_ref, out_ref):
    merge(heads, x_ref, s_ref[0], o_ref, lse_ref[...], out_ref, True)


def merge_last_kernel(heads, x_ref, out_ref):
    merge(heads, x_ref, None, None, None, out_ref, False)


def output_kernel(x_ref, w_ref, down_ref, up_ref, adapter_ref, out_ref):
    rows = x_ref.shape[0]
    i = lax.broadcasted_iota(jnp.int32, (rows, rows), 1)
    r = lax.broadcasted_iota(jnp.int32, (rows, rows), 0)
    near = NZM * NZP * NZH
    zh = lax.rem(i, NZH)
    zl = lax.rem(i // NZH, NZM * NZP)
    pick = jnp.where(r == (i // near) * near + zh * (NZM * NZP) + zl, 1.0, 0.0).astype(bf16)
    x = jnp.dot(pick, x_ref[...], preferred_element_type=f32).astype(bf16)
    plain = jnp.dot(x, w_ref[...], preferred_element_type=f32)
    narrow = jnp.dot(x, down_ref[...], preferred_element_type=f32)
    column = lax.broadcasted_iota(jnp.int32, narrow.shape, 1)
    narrow = jnp.where(column // LOW_RANK == adapter_ref[...], narrow, 0.0)
    out_ref[...] = plain + dot_fine(narrow, up_ref[...])


def cached_part(query, old_keys, old_values, old_length, last_key, last_value):
    group = HEADS // KV_HEADS
    q = query.reshape(-1, group, HEAD)
    kv = q.shape[0]
    scale = HEAD ** (-0.5)

    def score_of(keys):
        shaped = keys.reshape(keys.shape[0], kv, HEAD)
        return jnp.einsum("kgd,lkd->kgl", q, shaped, preferred_element_type=f32) * scale

    def mix_with(weights, values):
        shaped = values.reshape(values.shape[0], kv, HEAD)
        return jnp.einsum("kgl,lkd->kgd", weights, shaped, preferred_element_type=f32)

    valid = jnp.arange(old_keys.shape[0], dtype=jnp.int32) < old_length
    old = jnp.where(valid[None, None, :], score_of(old_keys), NEG)
    last = score_of(last_key[None, :])
    top = jnp.maximum(jnp.max(old, axis=-1, keepdims=True), last)
    old_w = jnp.exp(old - top)
    last_w = jnp.exp(last - top)
    total = jnp.sum(old_w, axis=-1, keepdims=True) + last_w
    o = mix_with((old_w / total).astype(bf16), old_values)
    o = o + mix_with((last_w / total).astype(bf16), last_value[None, :])
    lse = (top + jnp.log(total)).reshape(1, -1)
    return o.reshape(1, -1), jnp.pad(lse, ((0, 0), (0, HEAD - lse.shape[1])))


def per_device(
    prompt_activations,
    key_matrix,
    value_matrix,
    adapter_down_keyvalue,
    adapter_up_key,
    adapter_up_value,
    request_adapter,
    page_request,
    context_tokens,
    step_query,
    step_key,
    step_value,
    stored_keys,
    stored_values,
    output_matrix,
    adapter_down_output,
    adapter_up_output,
):
    device = lax.axis_index(DEV)
    me = lax.axis_index("x").astype(jnp.int32)
    parity = lax.axis_index("zp").astype(jnp.int32)
    zh = lax.axis_index("zh").astype(jnp.int32)
    tokens = prompt_activations.shape[0]
    pages = tokens // PAGE
    requests = request_adapter.shape[0]
    kv = key_matrix.shape[1] // HEAD
    heads = step_query.shape[1] // HEAD
    depth = key_matrix.shape[0]
    width = 2 * key_matrix.shape[1] + adapter_down_keyvalue.shape[1]

    weights = jnp.concatenate([key_matrix, value_matrix, adapter_down_keyvalue], axis=1)
    query_rows = jnp.pad(step_query.reshape(4, -1), ((0, 4), (0, width - step_query.shape[1] // 4)))
    block = jnp.concatenate([weights, query_rows], axis=0)
    column = lax.all_gather(block, Z8)
    count = column.shape[0]
    chunks = 2
    per_chunk = count // chunks
    pieces = []
    for c in range(chunks):
        part = column[c * per_chunk : (c + 1) * per_chunk]
        pieces.append(
            jnp.concatenate(
                [
                    part[:, :depth].reshape(per_chunk * depth, width),
                    part[:, depth : depth + 4].reshape(per_chunk * 4, width),
                ],
                axis=0,
            )
        )
    chunk_depth = per_chunk * depth

    mine, theirs = split_columns(prompt_activations, parity[None])
    theirs, pieces = lax.optimization_barrier((theirs, pieces))
    partner_act = swap_pair(theirs)

    by_offset = {0: pieces}
    ahead = behind = pieces
    for s in range(1, NX // 2 + 1):
        ahead = [ring_x(a, 1) for a in ahead]
        by_offset[NX - s] = ahead
        if 2 * s < NX:
            behind = [ring_x(b, -1) for b in behind]
            by_offset[s] = behind
    offsets = tuple(range(NX))
    flat = [a for off in offsets for a in by_offset[off]]

    quarter = step_query.shape[1] // 4
    own_queries = jnp.concatenate([a[chunk_depth:, :quarter] for a in flat], axis=0)
    pair_queries = swap_pair(own_queries)

    partial_other = project(partner_act, offsets, flat, chunk_depth, me[None], bf16)
    from_partner = swap_pair(partial_other)
    base = project(mine, offsets, flat, chunk_depth, me[None], f32)

    owners = page_request[:, 0]
    first_page = device * pages
    my_owners = lax.dynamic_slice_in_dim(owners, first_page, pages, 0)
    before = jnp.arange(owners.shape[0], dtype=jnp.int32)[None, :] < (
        first_page + jnp.arange(pages, dtype=jnp.int32)
    )[:, None]
    same = owners[None, :] == my_owners[:, None]
    rank = jnp.sum((same & before).astype(jnp.int32), axis=1)
    onehot = my_owners[:, None] == jnp.arange(requests, dtype=jnp.int32)[None, :]
    start = jnp.sum(jnp.where(onehot, context_tokens[None, :], 0), axis=1)
    adapter = jnp.sum(jnp.where(onehot, request_adapter[None, :], 0), axis=1)
    near = NZH * NZM * NZP
    z = my_owners % near
    z_low = z % (NZM * NZP)
    owner_spot = (my_owners // near) * near + z_low * NZH + z // (NZM * NZP)
    inside = jnp.arange(PAGE, dtype=jnp.int32)[None, :]
    position = ((start + rank * PAGE)[:, None] + inside).reshape(-1)
    token_adapter = jnp.broadcast_to(adapter[:, None], (pages, PAGE)).reshape(-1, 1)
    token_owner = jnp.broadcast_to(owner_spot[:, None], (pages, PAGE)).reshape(1, -1)
    half = HEAD // 2
    exponent = jnp.arange(half, dtype=f32) * (2.0 / HEAD)
    frequency = jnp.exp(-jnp.log(jnp.float32(rope_base)) * exponent)
    angles = position.astype(f32)[:, None] * frequency[None, :]
    cosine, sine = jnp.cos(angles), jnp.sin(angles)
    cosine = jnp.concatenate([cosine, cosine], axis=1)
    sine = jnp.concatenate([-sine, sine], axis=1)

    cache_o, cache_lse = cached_part(
        step_query[0],
        stored_keys[0],
        stored_values[0],
        jnp.sum(jnp.where(jnp.arange(requests) == device, context_tokens, 0)),
        step_key[0],
        step_value[0],
    )

    full_width = heads * HEAD + HEAD
    payload = pl.pallas_call(
        functools.partial(partial_kernel, heads, kv),
        in_specs=[SMEM] + [VMEM] * 10,
        out_specs=VMEM,
        out_shape=jax.ShapeDtypeStruct((requests, full_width), bf16),
        name="partial_attention",
    )(
        jnp.stack([me, parity]), base, from_partner, adapter_up_key, adapter_up_value,
        cosine, sine, token_adapter, token_owner, own_queries, pair_queries,
    )
    members = NX * NZM * NZP
    arrived = lax.all_to_all(payload.reshape(members, NZH, full_width), NEAR, 0, 0, tiled=True)
    merged = pl.pallas_call(
        functools.partial(merge_first_kernel, heads),
        in_specs=[SMEM] + [VMEM] * 3,
        out_specs=VMEM,
        out_shape=jax.ShapeDtypeStruct((8, full_width), bf16),
        name="merge_near",
    )(zh[None], arrived.reshape(members * NZH, full_width), cache_o, cache_lse)
    across = spread(merged[:NZH], "zh", NZH)
    mixed = pl.pallas_call(
        functools.partial(merge_last_kernel, heads),
        in_specs=[VMEM],
        out_specs=VMEM,
        out_shape=jax.ShapeDtypeStruct((8, heads * HEAD), bf16),
        name="merge_far",
    )(across.reshape(NZH * NZH, full_width))
    rows = spread(mixed[:NZH], NEAR, members).reshape(requests, heads * HEAD)
    partial_output = pl.pallas_call(
        output_kernel,
        in_specs=[VMEM] * 5,
        out_specs=VMEM,
        out_shape=jax.ShapeDtypeStruct((requests, output_matrix.shape[1]), f32),
        name="output_rows",
    )(rows, output_matrix, adapter_down_output, adapter_up_output, request_adapter[:, None])
    everything = spread(partial_output, "tp", lax.axis_size("tp"))
    return jnp.sum(everything, axis=0).astype(bf16)


def solution(mesh):
    finer = Mesh(
        mesh.devices.reshape(mesh.shape["group"], NX, NZH, NZM, NZP, mesh.shape["tp"]),
        ("group", "x", "zh", "zm", "zp", "tp"),
    )
    placed = (
        P(GROUP_DEV, None),
        P(DEV, "tp"),
        P(DEV, "tp"),
        P(DEV, None),
        P(None, "tp"),
        P(None, "tp"),
        P("group"),
        P("group", None),
        P("group"),
        P(GROUP_DEV, "tp"),
        P(GROUP_DEV, "tp"),
        P(GROUP_DEV, "tp"),
        P(GROUP_DEV, None, "tp"),
        P(GROUP_DEV, None, "tp"),
        P("tp", DEV),
        P("tp", None),
        P(None, DEV),
    )
    return jax.shard_map(
        per_device, mesh=finer, in_specs=placed, out_specs=P("group", DEV), check_vma=False
    )
```

```python
import functools

import jax
import jax.numpy as jnp
from jax import lax
from jax.experimental import pallas as pl
from jax.experimental.pallas import tpu as pltpu
from jax.sharding import Mesh
from jax.sharding import PartitionSpec as P


HEADS = 32
KV_HEADS = 4
HEAD = 128
LOW_RANK = 16
ADAPTER_COUNT = 4
PAGE = 4
LORA = ADAPTER_COUNT * LOW_RANK
DEV = ("x", "zh", "zm", "zp")
GROUP_DEV = ("group", "x", "zh", "zm", "zp")
Z8 = ("zh", "zm")
NEAR = ("x", "zm", "zp")
NX, NZH, NZM, NZP = 8, 4, 2, 2
NEG = -1e30

rope_base = 500000.0


f32 = jnp.float32
bf16 = jnp.bfloat16
SMEM = pl.BlockSpec(memory_space=pltpu.SMEM)
VMEM = pl.BlockSpec(memory_space=pltpu.VMEM)


def ring_x(x, step):
    return lax.ppermute(x, "x", [(i, (i + step) % NX) for i in range(NX)])


def swap_pair(x):
    return lax.ppermute(x, "zp", [(0, 1), (1, 0)])


def split_kernel(p_ref, a_ref, mine_ref, other_ref):
    parity = p_ref[0]
    half = HEAD // 2
    lane = lax.broadcasted_iota(jnp.int32, (a_ref.shape[0], HEAD), 1)
    low = lane < half
    first = parity == 0
    for k in range(mine_ref.shape[1] // HEAD):
        t0 = a_ref[:, 2 * k * HEAD : (2 * k + 1) * HEAD].astype(f32)
        t1 = a_ref[:, (2 * k + 1) * HEAD : (2 * k + 2) * HEAD].astype(f32)
        even = jnp.where(low, t0, pltpu.roll(t1, half, 1))
        odd = jnp.where(low, pltpu.roll(t0, half, 1), t1)
        cols = slice(k * HEAD, (k + 1) * HEAD)
        mine_ref[:, cols] = jnp.where(first, even, odd).astype(bf16)
        other_ref[:, cols] = jnp.where(first, odd, even).astype(bf16)


def split_columns(act, parity):
    rows, width = act.shape
    block = 64
    out = jax.ShapeDtypeStruct((rows, width // 2), bf16)
    return pl.pallas_call(
        split_kernel,
        grid=(rows // block,),
        in_specs=[SMEM, pl.BlockSpec((block, width), lambda i: (i, 0))],
        out_specs=[pl.BlockSpec((block, width // 2), lambda i: (i, 0))] * 2,
        out_shape=[out, out],
        name="split_columns",
    )(parity, act)


def project_kernel(offsets, chunks, depth, x_ref, a_ref, *refs):
    count = len(offsets) * chunks
    pieces, out_ref = refs[:count], refs[count]
    a_buf, w_buf, a_sem, w_sem = refs[count + 1 :]
    load_a = pltpu.make_async_copy(a_ref, a_buf, a_sem)
    load_a.start()
    loads = []
    for j in range(count):
        load = pltpu.make_async_copy(pieces[j].at[pl.ds(0, depth)], w_buf.at[j], w_sem.at[j])
        load.start()
        loads.append(load)
    me = x_ref[0]
    load_a.wait()
    total = jnp.zeros(out_ref.shape, f32)
    for i, off in enumerate(offsets):
        where = lax.rem(me + off, NX)
        for c in range(chunks):
            start = pl.multiple_of((where * chunks + c) * depth, depth)
            loads[i * chunks + c].wait()
            a = a_buf[:, pl.ds(start, depth)]
            total = total + jnp.dot(a, w_buf[i * chunks + c], preferred_element_type=f32)
    out_ref[...] = total.astype(out_ref.dtype)


def project(act, offsets, pieces, depth, me, dtype):
    chunks = len(pieces) // len(offsets)
    width = pieces[0].shape[1]
    anywhere = pl.BlockSpec(memory_space=pl.ANY)
    return pl.pallas_call(
        functools.partial(project_kernel, offsets, chunks, depth),
        in_specs=[SMEM] + [anywhere] * (1 + len(pieces)),
        out_specs=VMEM,
        out_shape=jax.ShapeDtypeStruct((act.shape[0], width), dtype),
        scratch_shapes=[
            pltpu.VMEM(act.shape, bf16),
            pltpu.VMEM((len(pieces), depth, width), bf16),
            pltpu.SemaphoreType.DMA,
            pltpu.SemaphoreType.DMA((len(pieces),)),
        ],
        name="project",
    )(me, act, *pieces)


def collect_kernel(*refs):
    out_ref = refs[-1]
    rows, width = refs[0].shape[0], out_ref.shape[1]
    for j, ref in enumerate(refs[:-1]):
        out_ref[j * rows : (j + 1) * rows, :] = ref[:, :width]


def collect_tails(pieces, depth, width):
    rows = pieces[0].shape[0] - depth
    tail = pl.BlockSpec((rows, pieces[0].shape[1]), lambda i: (depth // rows, 0))
    total = rows * len(pieces)
    return pl.pallas_call(
        collect_kernel,
        grid=(1,),
        in_specs=[tail] * len(pieces),
        out_specs=pl.BlockSpec((total, width), lambda i: (0, 0)),
        out_shape=jax.ShapeDtypeStruct((total, width), bf16),
        name="collect_tails",
    )(*pieces)


def two_terms(v):
    hi = v.astype(bf16)
    return hi, (v - hi.astype(f32)).astype(bf16)


def dot_fine(v, w):
    hi, lo = two_terms(v)
    return jnp.dot(hi, w, preferred_element_type=f32) + jnp.dot(lo, w, preferred_element_type=f32)


def three_terms(v):
    hi = v.astype(bf16).astype(f32)
    mid = (v - hi).astype(bf16).astype(f32)
    return hi, mid, v - hi - mid


def partial_kernel(
    heads, kv, s_ref, base_ref, other_ref, upk_ref, upv_ref, cos_ref, sin_ref,
    adapter_ref, owner_ref, q0_ref, q1_ref, out_ref,
):
    me, parity = s_ref[0], s_ref[1]
    tokens = base_ref.shape[0]
    rows = out_ref.shape[0]
    width = kv * HEAD
    raw = base_ref[...] + other_ref[...].astype(f32)
    column = lax.broadcasted_iota(jnp.int32, (tokens, 2 * LORA), 1)
    kept = lax.rem(column, LORA) // LOW_RANK == adapter_ref[...]
    chosen = jnp.where(kept, raw[:, 2 * width :], 0.0)
    key = raw[:, :width] + dot_fine(chosen[:, :LORA], upk_ref[...])
    value = (raw[:, width : 2 * width] + dot_fine(chosen[:, LORA:], upv_ref[...])).astype(bf16)
    turned = []
    for k in range(kv):
        part = key[:, k * HEAD : (k + 1) * HEAD]
        spun = part * cos_ref[...] + pltpu.roll(part, HEAD // 2, 1) * sin_ref[...]
        turned.append(spun.astype(bf16))
    source = q0_ref.shape[0]
    blocks = 4
    i = lax.broadcasted_iota(jnp.int32, (rows, source), 1)
    row = lax.broadcasted_iota(jnp.int32, (rows, source), 0)
    row_half = lax.rem(row // NZH, 2)
    row_base = row - row_half * NZH
    block = lax.rem(i, blocks)
    z8 = lax.rem(i // blocks, NZH * NZM)
    off = i // (blocks * NZH * NZM)
    xs = lax.rem(off + me, NX)
    spot = (xs * (NZM * NZP) + lax.rem(z8, NZM) * NZP) * (2 * NZH) + z8 // NZM
    hit0 = row_base == spot + parity * (2 * NZH)
    hit1 = row_base == spot + (1 - parity) * (2 * NZH)
    queries = []
    for g in range(2):
        right = block == 2 * row_half + g
        pick0 = jnp.where(hit0 & right, 1.0, 0.0).astype(bf16)
        pick1 = jnp.where(hit1 & right, 1.0, 0.0).astype(bf16)
        got = jnp.dot(pick0, q0_ref[...], preferred_element_type=f32) + jnp.dot(
            pick1, q1_ref[...], preferred_element_type=f32
        )
        queries.append(got.astype(bf16))
    t_row = lax.broadcasted_iota(jnp.int32, (rows, tokens), 0)
    t_first = lax.rem(t_row // NZH, 2) == 0
    mask = t_row - jnp.where(t_first, 0, NZH) == owner_ref[...]
    lane = lax.broadcasted_iota(jnp.int32, (rows, HEAD), 1)
    stat = jnp.zeros((rows, HEAD), f32)
    across = (((1,), (1,)), ((), ()))
    for h in range(heads):
        q = queries[h // 4][:, (h % 4) * HEAD : (h % 4 + 1) * HEAD]
        s0 = lax.dot_general(q, turned[0], across, preferred_element_type=f32)
        s1 = lax.dot_general(q, turned[1], across, preferred_element_type=f32)
        s = jnp.where(mask, jnp.where(t_first, s0, s1) * (HEAD ** (-0.5)), NEG)
        top = jnp.max(s, axis=1, keepdims=True)
        e = jnp.where(mask, jnp.exp(s - top), 0.0)
        total = jnp.sum(e, axis=1, keepdims=True)
        e0 = jnp.where(t_first, e, 0.0).astype(bf16)
        e1 = jnp.where(t_first, 0.0, e).astype(bf16)
        o = jnp.dot(e0, value[:, :HEAD], preferred_element_type=f32) + jnp.dot(
            e1, value[:, HEAD:], preferred_element_type=f32
        )
        full = total > 0.0
        o = o * jnp.where(full, 1.0 / jnp.maximum(total, 1e-30), 0.0)
        out_ref[:, h * HEAD : (h + 1) * HEAD] = o.astype(bf16)
        lse = jnp.where(full, top + jnp.log(jnp.maximum(total, 1e-30)), NEG)
        hi, mid, lo = three_terms(lse)
        stat = jnp.where(lane == h, hi, stat)
        stat = jnp.where(lane == heads + h, mid, stat)
        stat = jnp.where(lane == 2 * heads + h, lo, stat)
    out_ref[:, heads * HEAD :] = stat.astype(bf16)


def reduce_rows(v, op):
    while v.shape[0] > 8:
        half = v.shape[0] // 2
        v = op(v[:half], v[half:])
    return v


def merge(heads, x_ref, cached, out_ref, with_stat):
    rows = x_ref.shape[0]
    copies = out_ref.shape[0] // 8
    st = x_ref[:, heads * HEAD :].astype(f32)
    lse = st + pltpu.roll(st, HEAD - heads, 1) + pltpu.roll(st, HEAD - 2 * heads, 1)
    lane = lax.broadcasted_iota(jnp.int32, (rows, HEAD), 1)
    lse = jnp.where(lane < heads, lse, 0.0)
    top = reduce_rows(lse, jnp.maximum)
    if cached is not None:
        zh, o_ref, lse_ref = cached
        row = lax.broadcasted_iota(jnp.int32, (8, HEAD), 0)
        first = row < NZH
        here = lax.rem(row, NZH) == zh
        cache_lse = jnp.where(first, lse_ref[0:1, :], lse_ref[1:2, :])
        top = jnp.where(here, jnp.maximum(top, cache_lse), top)
        cache_w = jnp.where(here, jnp.exp(cache_lse - top), 0.0)
    w = jnp.exp(lse - jnp.tile(top, (rows // 8, 1)))
    total = reduce_rows(w, jnp.add)
    if cached is not None:
        total = total + cache_w
    for h in range(heads):
        cols = slice(h * HEAD, (h + 1) * HEAD)
        o = reduce_rows(w[:, h : h + 1] * x_ref[:, cols].astype(f32), jnp.add)
        if cached is not None:
            kept = jnp.where(first, o_ref[0:1, cols], o_ref[1:2, cols])
            o = o + cache_w[:, h : h + 1] * kept
        o = (o / total[:, h : h + 1]).astype(bf16)
        for c in range(copies):
            out_ref[c * 8 : (c + 1) * 8, cols] = o
    if with_stat:
        final = top + jnp.log(total)
        hi, mid, lo = three_terms(jnp.where(lane[:8] < heads, final, 0.0))
        stat = hi + pltpu.roll(mid, heads, 1) + pltpu.roll(lo, 2 * heads, 1)
        for c in range(copies):
            out_ref[c * 8 : (c + 1) * 8, heads * HEAD :] = stat.astype(bf16)


def merge_near_kernel(heads, s_ref, x_ref, o_ref, lse_ref, out_ref):
    merge(heads, x_ref, (s_ref[0], o_ref, lse_ref), out_ref, True)


def merge_far_kernel(heads, x_ref, out_ref):
    merge(heads, x_ref, None, out_ref, False)


def output_kernel(x_ref, w_ref, down_ref, up_ref, adapter_ref, out_ref):
    rows = adapter_ref.shape[1]
    half_width = x_ref.shape[1]
    i = lax.broadcasted_iota(jnp.int32, (rows, x_ref.shape[0]), 1)
    r = lax.broadcasted_iota(jnp.int32, (rows, x_ref.shape[0]), 0)
    near = NZM * NZP
    member = i // (2 * NZH)
    hit = r == (member // near) * (near * NZH) + lax.rem(i, NZH) * near + lax.rem(member, near)
    half = lax.rem(i // NZH, 2)
    across = (((1,), (1,)), ((), ()))
    plain = jnp.zeros((w_ref.shape[0], rows), f32)
    narrow = jnp.zeros((down_ref.shape[0], rows), f32)
    for k in range(2):
        pick = jnp.where(hit & (half == k), 1.0, 0.0).astype(bf16)
        x = jnp.dot(pick, x_ref[...], preferred_element_type=f32).astype(bf16)
        cols = slice(k * half_width, (k + 1) * half_width)
        plain = plain + lax.dot_general(w_ref[:, cols], x, across, preferred_element_type=f32)
        narrow = narrow + lax.dot_general(down_ref[:, cols], x, across, preferred_element_type=f32)
    column = lax.broadcasted_iota(jnp.int32, narrow.shape, 0)
    hi, lo = two_terms(jnp.where(column // LOW_RANK == adapter_ref[...], narrow, 0.0))
    up = up_ref[...]
    plain = plain + (
        jnp.dot(up, hi, preferred_element_type=f32) + jnp.dot(up, lo, preferred_element_type=f32)
    )
    count = w_ref.shape[0]
    for c in range(out_ref.shape[0] // count):
        out_ref[c * count : (c + 1) * count, :] = plain


def cached_part(query, old_keys, old_values, old_length, last_key, last_value):
    group = HEADS // KV_HEADS
    q = query.reshape(-1, group, HEAD)
    kv = q.shape[0]
    scale = HEAD ** (-0.5)

    def score_of(keys):
        shaped = keys.reshape(keys.shape[0], kv, HEAD)
        return jnp.einsum("kgd,lkd->kgl", q, shaped, preferred_element_type=f32) * scale

    def mix_with(weights, values):
        shaped = values.reshape(values.shape[0], kv, HEAD)
        return jnp.einsum("kgl,lkd->kgd", weights, shaped, preferred_element_type=f32)

    valid = jnp.arange(old_keys.shape[0], dtype=jnp.int32) < old_length
    old = jnp.where(valid[None, None, :], score_of(old_keys), NEG)
    last = score_of(last_key[None, :])
    top = jnp.maximum(jnp.max(old, axis=-1, keepdims=True), last)
    old_w = jnp.exp(old - top)
    last_w = jnp.exp(last - top)
    total = jnp.sum(old_w, axis=-1, keepdims=True) + last_w
    o = mix_with((old_w / total).astype(bf16), old_values)
    o = o + mix_with((last_w / total).astype(bf16), last_value[None, :])
    lse = (top + jnp.log(total)).reshape(kv, -1)
    return o.reshape(kv, -1), jnp.pad(lse, ((0, 0), (0, HEAD - lse.shape[1])))


def per_device(
    prompt_activations,
    key_matrix,
    value_matrix,
    adapter_down_keyvalue,
    adapter_up_key,
    adapter_up_value,
    request_adapter,
    page_request,
    context_tokens,
    step_query,
    step_key,
    step_value,
    stored_keys,
    stored_values,
    output_matrix,
    adapter_down_output,
    adapter_up_output,
):
    device = lax.axis_index(DEV)
    me = lax.axis_index("x").astype(jnp.int32)
    parity = lax.axis_index("zp").astype(jnp.int32)
    zh = lax.axis_index("zh").astype(jnp.int32)
    tokens = prompt_activations.shape[0]
    pages = tokens // PAGE
    requests = request_adapter.shape[0]
    kv = key_matrix.shape[1] // HEAD
    heads = step_query.shape[1] // HEAD
    depth = key_matrix.shape[0]
    width = 2 * key_matrix.shape[1] + adapter_down_keyvalue.shape[1]

    weights = jnp.concatenate([key_matrix, value_matrix, adapter_down_keyvalue], axis=1)
    query_rows = jnp.pad(step_query.reshape(4, -1), ((0, 4), (0, width - step_query.shape[1] // 4)))
    block = jnp.concatenate([weights, query_rows], axis=0)
    column = lax.all_gather(block, Z8)
    count = column.shape[0]
    chunks = 2
    per_chunk = count // chunks
    pieces = []
    for c in range(chunks):
        part = column[c * per_chunk : (c + 1) * per_chunk]
        pieces.append(
            jnp.concatenate(
                [
                    part[:, :depth].reshape(per_chunk * depth, width),
                    part[:, depth : depth + 4].reshape(per_chunk * 4, width),
                ],
                axis=0,
            )
        )
    chunk_depth = per_chunk * depth

    activations, _ = lax.optimization_barrier((prompt_activations, column))
    mine, theirs = split_columns(activations, parity[None])
    partner_act = swap_pair(theirs)

    by_offset = {0: pieces}
    ahead = behind = pieces
    for s in range(1, NX // 2):
        ahead = [ring_x(a, 1) for a in ahead]
        behind = [ring_x(b, -1) for b in behind]
        by_offset[NX - s] = ahead
        by_offset[s] = behind
    by_offset[NX // 2] = [ring_x(ahead[0], 1), ring_x(behind[1], -1)]
    offsets = (0, 7, 1, 6, 2, 5, 3, 4)
    flat = [a for off in range(NX) for a in by_offset[off]]
    ordered = [a for off in offsets for a in by_offset[off]]

    quarter = step_query.shape[1] // 4
    own_queries = collect_tails(flat, chunk_depth, quarter)
    pair_queries = swap_pair(own_queries)

    partial_other = project(partner_act, offsets, ordered, chunk_depth, me[None], bf16)
    from_partner = swap_pair(partial_other)
    base = project(mine, offsets, ordered, chunk_depth, me[None], f32)

    owners = page_request[:, 0]
    first_page = device * pages
    my_owners = lax.dynamic_slice_in_dim(owners, first_page, pages, 0)
    before = jnp.arange(owners.shape[0], dtype=jnp.int32)[None, :] < (
        first_page + jnp.arange(pages, dtype=jnp.int32)
    )[:, None]
    same = owners[None, :] == my_owners[:, None]
    rank = jnp.sum((same & before).astype(jnp.int32), axis=1)
    onehot = my_owners[:, None] == jnp.arange(requests, dtype=jnp.int32)[None, :]
    start = jnp.sum(jnp.where(onehot, context_tokens[None, :], 0), axis=1)
    adapter = jnp.sum(jnp.where(onehot, request_adapter[None, :], 0), axis=1)
    near = NZH * NZM * NZP
    z = my_owners % near
    z_low = z % (NZM * NZP)
    owner_spot = ((my_owners // near) * (NZM * NZP) + z_low) * (2 * NZH) + z // (NZM * NZP)
    inside = jnp.arange(PAGE, dtype=jnp.int32)[None, :]
    position = ((start + rank * PAGE)[:, None] + inside).reshape(-1)
    token_adapter = jnp.broadcast_to(adapter[:, None], (pages, PAGE)).reshape(-1, 1)
    token_owner = jnp.broadcast_to(owner_spot[:, None], (pages, PAGE)).reshape(1, -1)
    half = HEAD // 2
    exponent = jnp.arange(half, dtype=f32) * (2.0 / HEAD)
    frequency = jnp.exp(-jnp.log(jnp.float32(rope_base)) * exponent)
    angles = position.astype(f32)[:, None] * frequency[None, :]
    cosine, sine = jnp.cos(angles), jnp.sin(angles)
    cosine = jnp.concatenate([cosine, cosine], axis=1)
    sine = jnp.concatenate([-sine, sine], axis=1)

    cache_o, cache_lse = cached_part(
        step_query[0],
        stored_keys[0],
        stored_values[0],
        jnp.sum(jnp.where(jnp.arange(requests) == device, context_tokens, 0)),
        step_key[0],
        step_value[0],
    )

    half_heads = heads // kv
    half_width = half_heads * HEAD
    full_width = half_width + HEAD
    members = NX * NZM * NZP
    unit = kv * NZH
    payload = pl.pallas_call(
        functools.partial(partial_kernel, half_heads, kv),
        in_specs=[SMEM] + [VMEM] * 10,
        out_specs=VMEM,
        out_shape=jax.ShapeDtypeStruct((members * unit, full_width), bf16),
        name="partial_attention",
    )(
        jnp.stack([me, parity]), base, from_partner, adapter_up_key, adapter_up_value,
        cosine, sine, token_adapter, token_owner, own_queries, pair_queries,
    )
    arrived = lax.all_to_all(payload.reshape(members, unit, full_width), NEAR, 0, 0, tiled=True)
    merged = pl.pallas_call(
        functools.partial(merge_near_kernel, half_heads),
        in_specs=[SMEM] + [VMEM] * 3,
        out_specs=VMEM,
        out_shape=jax.ShapeDtypeStruct((NZH * unit, full_width), bf16),
        name="merge_near",
    )(zh[None], arrived.reshape(members * unit, full_width), cache_o, cache_lse)
    across = lax.all_to_all(merged.reshape(NZH, unit, full_width), "zh", 0, 0, tiled=True)
    mixed = pl.pallas_call(
        functools.partial(merge_far_kernel, half_heads),
        in_specs=[VMEM],
        out_specs=VMEM,
        out_shape=jax.ShapeDtypeStruct((members * unit, half_width), bf16),
        name="merge_far",
    )(across.reshape(NZH * unit, full_width))
    rows = lax.all_to_all(mixed.reshape(members, unit, half_width), NEAR, 0, 0, tiled=True)
    pair = lax.axis_size("tp")
    columns = output_matrix.shape[1]
    partial_output = pl.pallas_call(
        output_kernel,
        in_specs=[VMEM] * 5,
        out_specs=VMEM,
        out_shape=jax.ShapeDtypeStruct((pair * columns, requests), f32),
        name="output_rows",
    )(
        rows.reshape(members * unit, half_width), output_matrix.T, adapter_down_output.T,
        adapter_up_output.T, request_adapter[None, :],
    )
    everything = lax.all_to_all(
        partial_output.reshape(pair, columns, requests), "tp", 0, 0, tiled=True
    )
    return jnp.sum(everything, axis=0).T.astype(bf16)


def solution(mesh):
    finer = Mesh(
        mesh.devices.reshape(mesh.shape["group"], NX, NZH, NZM, NZP, mesh.shape["tp"]),
        ("group", "x", "zh", "zm", "zp", "tp"),
    )
    placed = (
        P(GROUP_DEV, None),
        P(DEV, "tp"),
        P(DEV, "tp"),
        P(DEV, None),
        P(None, "tp"),
        P(None, "tp"),
        P("group"),
        P("group", None),
        P("group"),
        P(GROUP_DEV, "tp"),
        P(GROUP_DEV, "tp"),
        P(GROUP_DEV, "tp"),
        P(GROUP_DEV, None, "tp"),
        P(GROUP_DEV, None, "tp"),
        P("tp", DEV),
        P("tp", None),
        P(None, DEV),
    )
    return jax.shard_map(
        per_device, mesh=finer, in_specs=placed, out_specs=P("group", DEV), check_vma=False
    )
```

```python
import functools

import jax
import jax.numpy as jnp
from jax import lax
from jax.experimental import pallas as pl
from jax.experimental.pallas import tpu as pltpu
from jax.sharding import Mesh
from jax.sharding import PartitionSpec as P


HEADS = 32
KV_HEADS = 4
HEAD = 128
LOW_RANK = 16
ADAPTER_COUNT = 4
PAGE = 4
LORA = ADAPTER_COUNT * LOW_RANK
DEV = ("x", "zh", "zm", "zp")
GROUP_DEV = ("group", "x", "zh", "zm", "zp")
Z8 = ("zh", "zm")
NEAR = ("x", "zm", "zp")
NX, NZH, NZM, NZP = 8, 4, 2, 2
NEG = -1e30

rope_base = 500000.0


f32 = jnp.float32
bf16 = jnp.bfloat16
SMEM = pl.BlockSpec(memory_space=pltpu.SMEM)
VMEM = pl.BlockSpec(memory_space=pltpu.VMEM)


def room(mib):
    return pltpu.CompilerParams(vmem_limit_bytes=mib * 1024 * 1024)


def ring_x(x, step):
    return lax.ppermute(x, "x", [(i, (i + step) % NX) for i in range(NX)])


def swap_pair(x):
    return lax.ppermute(x, "zp", [(0, 1), (1, 0)])


def split_kernel(p_ref, a_ref, mine_ref, other_ref):
    half = HEAD // 2

    def write(even_ref, odd_ref):
        for k in range(even_ref.shape[1] // HEAD):
            t0 = a_ref[:, 2 * k * HEAD : (2 * k + 1) * HEAD]
            t1 = a_ref[:, (2 * k + 1) * HEAD : (2 * k + 2) * HEAD]
            cols = slice(k * HEAD, (k + 1) * HEAD)
            even_ref[:, cols] = jnp.concatenate([t0[:, :half], t1[:, :half]], axis=1)
            odd_ref[:, cols] = jnp.concatenate([t0[:, half:], t1[:, half:]], axis=1)

    @pl.when(p_ref[0] == 0)
    def _():
        write(mine_ref, other_ref)

    @pl.when(p_ref[0] != 0)
    def _():
        write(other_ref, mine_ref)


def split_columns(act, parity):
    rows, width = act.shape
    block = 32
    out = jax.ShapeDtypeStruct((rows, width // 2), bf16)
    return pl.pallas_call(
        split_kernel,
        grid=(rows // block,),
        in_specs=[SMEM, pl.BlockSpec((block, width), lambda i: (i, 0))],
        out_specs=[pl.BlockSpec((block, width // 2), lambda i: (i, 0))] * 2,
        out_shape=[out, out],
        compiler_params=room(8),
        name="split_columns",
    )(parity, act)


def project_kernel(offsets, chunks, depth, x_ref, a_ref, *refs):
    pieces, out_ref = refs[:-1], refs[-1]
    me = x_ref[0]
    total = None
    for i, off in enumerate(offsets):
        where = lax.rem(me + off, NX)
        start = pl.multiple_of(where * chunks * depth, chunks * depth)
        a = a_ref[:, pl.ds(start, chunks * depth)]
        w = jnp.concatenate(
            [pieces[i * chunks + c][0:depth, :] for c in range(chunks)], axis=0
        )
        part = jnp.dot(a, w, preferred_element_type=f32)
        total = part if total is None else total + part
    out_ref[...] = total.astype(out_ref.dtype)


def project(act, offsets, pieces, depth, me, dtype):
    chunks = len(pieces) // len(offsets)
    width = pieces[0].shape[1]
    return pl.pallas_call(
        functools.partial(project_kernel, offsets, chunks, depth),
        in_specs=[SMEM] + [VMEM] * (1 + len(pieces)),
        out_specs=VMEM,
        out_shape=jax.ShapeDtypeStruct((act.shape[0], width), dtype),
        compiler_params=room(20),
        name="project",
    )(me, act, *pieces)


def collect_kernel(after_ref, *refs):
    out_ref = refs[-1]
    rows, width = refs[0].shape[0], out_ref.shape[1]
    for j, ref in enumerate(refs[:-1]):
        out_ref[j * rows : (j + 1) * rows, :] = ref[:, :width]


def collect_tails(pieces, depth, width, after):
    rows = pieces[0].shape[0] - depth
    tail = pl.BlockSpec((rows, pieces[0].shape[1]), lambda i: (depth // rows, 0))
    total = rows * len(pieces)
    return pl.pallas_call(
        collect_kernel,
        grid=(1,),
        in_specs=[pl.BlockSpec(memory_space=pl.ANY)] + [tail] * len(pieces),
        out_specs=pl.BlockSpec((total, width), lambda i: (0, 0)),
        out_shape=jax.ShapeDtypeStruct((total, width), bf16),
        compiler_params=room(8),
        name="collect_tails",
    )(after, *pieces)


def two_terms(v):
    hi = v.astype(bf16)
    return hi, (v - hi.astype(f32)).astype(bf16)


def dot_fine(v, w):
    hi, lo = two_terms(v)
    return jnp.dot(hi, w, preferred_element_type=f32) + jnp.dot(lo, w, preferred_element_type=f32)


def three_terms(v):
    hi = v.astype(bf16).astype(f32)
    mid = (v - hi).astype(bf16).astype(f32)
    return hi, mid, v - hi - mid


def partial_kernel(
    heads, kv, s_ref, base_ref, other_ref, upk_ref, upv_ref, cos_ref, sin_ref,
    adapter_ref, owner_ref, q0_ref, q1_ref, out_ref,
):
    me, parity = s_ref[0], s_ref[1]
    tokens = base_ref.shape[0]
    rows = out_ref.shape[0]
    width = kv * HEAD
    raw = base_ref[...] + other_ref[...].astype(f32)
    column = lax.broadcasted_iota(jnp.int32, (tokens, 2 * LORA), 1)
    kept = lax.rem(column, LORA) // LOW_RANK == adapter_ref[...]
    chosen = jnp.where(kept, raw[:, 2 * width :], 0.0)
    key = raw[:, :width] + dot_fine(chosen[:, :LORA], upk_ref[...])
    value = (raw[:, width : 2 * width] + dot_fine(chosen[:, LORA:], upv_ref[...])).astype(bf16)
    turned = []
    for k in range(kv):
        part = key[:, k * HEAD : (k + 1) * HEAD]
        spun = part * cos_ref[...] + pltpu.roll(part, HEAD // 2, 1) * sin_ref[...]
        turned.append(spun.astype(bf16))
    source = q0_ref.shape[0]
    blocks = 4
    i = lax.broadcasted_iota(jnp.int32, (rows, source), 1)
    row = lax.broadcasted_iota(jnp.int32, (rows, source), 0)
    row_half = lax.rem(row // NZH, 2)
    row_base = row - row_half * NZH
    block = lax.rem(i, blocks)
    z8 = lax.rem(i // blocks, NZH * NZM)
    off = i // (blocks * NZH * NZM)
    xs = lax.rem(off + me, NX)
    spot = (xs * (NZM * NZP) + lax.rem(z8, NZM) * NZP) * (2 * NZH) + z8 // NZM
    hit0 = row_base == spot + parity * (2 * NZH)
    hit1 = row_base == spot + (1 - parity) * (2 * NZH)
    queries = []
    for g in range(2):
        right = block == 2 * row_half + g
        pick0 = jnp.where(hit0 & right, 1.0, 0.0).astype(bf16)
        pick1 = jnp.where(hit1 & right, 1.0, 0.0).astype(bf16)
        got = jnp.dot(pick0, q0_ref[...], preferred_element_type=f32) + jnp.dot(
            pick1, q1_ref[...], preferred_element_type=f32
        )
        queries.append(got.astype(bf16))
    t_row = lax.broadcasted_iota(jnp.int32, (rows, tokens), 0)
    t_first = lax.rem(t_row // NZH, 2) == 0
    mask = t_row - jnp.where(t_first, 0, NZH) == owner_ref[...]
    lane = lax.broadcasted_iota(jnp.int32, (rows, HEAD), 1)
    stat = jnp.zeros((rows, HEAD), f32)
    across = (((1,), (1,)), ((), ()))
    for h in range(heads):
        q = queries[h // 4][:, (h % 4) * HEAD : (h % 4 + 1) * HEAD]
        s0 = lax.dot_general(q, turned[0], across, preferred_element_type=f32)
        s1 = lax.dot_general(q, turned[1], across, preferred_element_type=f32)
        s = jnp.where(mask, jnp.where(t_first, s0, s1) * (HEAD ** (-0.5)), NEG)
        top = jnp.max(s, axis=1, keepdims=True)
        e = jnp.where(mask, jnp.exp(s - top), 0.0)
        total = jnp.sum(e, axis=1, keepdims=True)
        e0 = jnp.where(t_first, e, 0.0).astype(bf16)
        e1 = jnp.where(t_first, 0.0, e).astype(bf16)
        o = jnp.dot(e0, value[:, :HEAD], preferred_element_type=f32) + jnp.dot(
            e1, value[:, HEAD:], preferred_element_type=f32
        )
        full = total > 0.0
        o = o * jnp.where(full, 1.0 / jnp.maximum(total, 1e-30), 0.0)
        out_ref[:, h * HEAD : (h + 1) * HEAD] = o.astype(bf16)
        lse = jnp.where(full, top + jnp.log(jnp.maximum(total, 1e-30)), NEG)
        hi, mid, lo = three_terms(lse)
        stat = jnp.where(lane == h, hi, stat)
        stat = jnp.where(lane == heads + h, mid, stat)
        stat = jnp.where(lane == 2 * heads + h, lo, stat)
    out_ref[:, heads * HEAD :] = stat.astype(bf16)


def reduce_rows(v, op):
    while v.shape[0] > 8:
        half = v.shape[0] // 2
        v = op(v[:half], v[half:])
    return v


def merge(heads, x_ref, cached, out_ref, with_stat):
    rows = x_ref.shape[0]
    copies = out_ref.shape[0] // 8
    st = x_ref[:, heads * HEAD :].astype(f32)
    lse = st + pltpu.roll(st, HEAD - heads, 1) + pltpu.roll(st, HEAD - 2 * heads, 1)
    lane = lax.broadcasted_iota(jnp.int32, (rows, HEAD), 1)
    lse = jnp.where(lane < heads, lse, 0.0)
    top = reduce_rows(lse, jnp.maximum)
    if cached is not None:
        zh, o_ref, lse_ref = cached
        row = lax.broadcasted_iota(jnp.int32, (8, HEAD), 0)
        first = row < NZH
        here = lax.rem(row, NZH) == zh
        cache_lse = jnp.where(first, lse_ref[0:1, :], lse_ref[1:2, :])
        top = jnp.where(here, jnp.maximum(top, cache_lse), top)
        cache_w = jnp.where(here, jnp.exp(cache_lse - top), 0.0)
    w = jnp.exp(lse - jnp.tile(top, (rows // 8, 1)))
    total = reduce_rows(w, jnp.add)
    if cached is not None:
        total = total + cache_w
    for h in range(heads):
        cols = slice(h * HEAD, (h + 1) * HEAD)
        o = reduce_rows(w[:, h : h + 1] * x_ref[:, cols].astype(f32), jnp.add)
        if cached is not None:
            kept = jnp.where(first, o_ref[0:1, cols], o_ref[1:2, cols])
            o = o + cache_w[:, h : h + 1] * kept
        o = (o / total[:, h : h + 1]).astype(bf16)
        for c in range(copies):
            out_ref[c * 8 : (c + 1) * 8, cols] = o
    if with_stat:
        final = top + jnp.log(total)
        hi, mid, lo = three_terms(jnp.where(lane[:8] < heads, final, 0.0))
        stat = hi + pltpu.roll(mid, heads, 1) + pltpu.roll(lo, 2 * heads, 1)
        for c in range(copies):
            out_ref[c * 8 : (c + 1) * 8, heads * HEAD :] = stat.astype(bf16)


def merge_near_kernel(heads, s_ref, x_ref, o_ref, lse_ref, out_ref):
    merge(heads, x_ref, (s_ref[0], o_ref, lse_ref), out_ref, True)


def merge_far_kernel(heads, x_ref, out_ref):
    merge(heads, x_ref, None, out_ref, False)


def output_kernel(x_ref, w_ref, down_ref, up_ref, adapter_ref, out_ref):
    rows = adapter_ref.shape[1]
    half_width = x_ref.shape[1]
    i = lax.broadcasted_iota(jnp.int32, (rows, x_ref.shape[0]), 1)
    r = lax.broadcasted_iota(jnp.int32, (rows, x_ref.shape[0]), 0)
    near = NZM * NZP
    member = i // (2 * NZH)
    hit = r == (member // near) * (near * NZH) + lax.rem(i, NZH) * near + lax.rem(member, near)
    half = lax.rem(i // NZH, 2)
    across = (((1,), (1,)), ((), ()))
    plain = jnp.zeros((w_ref.shape[0], rows), f32)
    narrow = jnp.zeros((down_ref.shape[0], rows), f32)
    for k in range(2):
        pick = jnp.where(hit & (half == k), 1.0, 0.0).astype(bf16)
        x = jnp.dot(pick, x_ref[...], preferred_element_type=f32).astype(bf16)
        cols = slice(k * half_width, (k + 1) * half_width)
        plain = plain + lax.dot_general(w_ref[:, cols], x, across, preferred_element_type=f32)
        narrow = narrow + lax.dot_general(down_ref[:, cols], x, across, preferred_element_type=f32)
    column = lax.broadcasted_iota(jnp.int32, narrow.shape, 0)
    hi, lo = two_terms(jnp.where(column // LOW_RANK == adapter_ref[...], narrow, 0.0))
    up = up_ref[...]
    plain = plain + (
        jnp.dot(up, hi, preferred_element_type=f32) + jnp.dot(up, lo, preferred_element_type=f32)
    )
    count = w_ref.shape[0]
    for c in range(out_ref.shape[0] // count):
        out_ref[c * count : (c + 1) * count, :] = plain


def cached_part(query, old_keys, old_values, old_length, last_key, last_value):
    group = HEADS // KV_HEADS
    q = query.reshape(-1, group, HEAD)
    kv = q.shape[0]
    scale = HEAD ** (-0.5)

    def score_of(keys):
        shaped = keys.reshape(keys.shape[0], kv, HEAD)
        return jnp.einsum("kgd,lkd->kgl", q, shaped, preferred_element_type=f32) * scale

    def mix_with(weights, values):
        shaped = values.reshape(values.shape[0], kv, HEAD)
        return jnp.einsum("kgl,lkd->kgd", weights, shaped, preferred_element_type=f32)

    valid = jnp.arange(old_keys.shape[0], dtype=jnp.int32) < old_length
    old = jnp.where(valid[None, None, :], score_of(old_keys), NEG)
    last = score_of(last_key[None, :])
    top = jnp.maximum(jnp.max(old, axis=-1, keepdims=True), last)
    old_w = jnp.exp(old - top)
    last_w = jnp.exp(last - top)
    total = jnp.sum(old_w, axis=-1, keepdims=True) + last_w
    o = mix_with((old_w / total).astype(bf16), old_values)
    o = o + mix_with((last_w / total).astype(bf16), last_value[None, :])
    lse = (top + jnp.log(total)).reshape(kv, -1)
    return o.reshape(kv, -1), jnp.pad(lse, ((0, 0), (0, HEAD - lse.shape[1])))


def per_device(
    prompt_activations,
    key_matrix,
    value_matrix,
    adapter_down_keyvalue,
    adapter_up_key,
    adapter_up_value,
    request_adapter,
    page_request,
    context_tokens,
    step_query,
    step_key,
    step_value,
    stored_keys,
    stored_values,
    output_matrix,
    adapter_down_output,
    adapter_up_output,
):
    device = lax.axis_index(DEV)
    me = lax.axis_index("x").astype(jnp.int32)
    parity = lax.axis_index("zp").astype(jnp.int32)
    zh = lax.axis_index("zh").astype(jnp.int32)
    tokens = prompt_activations.shape[0]
    pages = tokens // PAGE
    requests = request_adapter.shape[0]
    kv = key_matrix.shape[1] // HEAD
    heads = step_query.shape[1] // HEAD
    depth = key_matrix.shape[0]
    width = 2 * key_matrix.shape[1] + adapter_down_keyvalue.shape[1]

    weights = jnp.concatenate([key_matrix, value_matrix, adapter_down_keyvalue], axis=1)
    query_rows = jnp.pad(step_query.reshape(4, -1), ((0, 4), (0, width - step_query.shape[1] // 4)))
    block = jnp.concatenate([weights, query_rows], axis=0)
    column = lax.all_gather(block, Z8)
    count = column.shape[0]
    chunks = 2
    per_chunk = count // chunks
    pieces = []
    for c in range(chunks):
        part = column[c * per_chunk : (c + 1) * per_chunk]
        pieces.append(
            jnp.concatenate(
                [
                    part[:, :depth].reshape(per_chunk * depth, width),
                    part[:, depth : depth + 4].reshape(per_chunk * 4, width),
                ],
                axis=0,
            )
        )
    chunk_depth = per_chunk * depth

    activations, _ = lax.optimization_barrier((prompt_activations, column))
    mine, theirs = split_columns(activations, parity[None])
    partner_act = swap_pair(theirs)

    by_offset = {0: pieces}
    ahead = behind = pieces
    for s in range(1, NX // 2):
        ahead = [ring_x(a, 1) for a in ahead]
        behind = [ring_x(b, -1) for b in behind]
        by_offset[NX - s] = ahead
        by_offset[s] = behind
    by_offset[NX // 2] = [ring_x(ahead[0], 1), ring_x(behind[1], -1)]
    offsets = (0, 7, 1, 6, 2, 5, 3, 4)
    flat = [a for off in range(NX) for a in by_offset[off]]
    ordered = [a for off in offsets for a in by_offset[off]]

    quarter = step_query.shape[1] // 4
    partial_other = project(partner_act, offsets, ordered, chunk_depth, me[None], bf16)
    from_partner = swap_pair(partial_other)
    own_queries = collect_tails(flat, chunk_depth, quarter, partial_other)
    pair_queries = swap_pair(own_queries)
    base = project(mine, offsets, ordered, chunk_depth, me[None], f32)

    owners = page_request[:, 0]
    first_page = device * pages
    my_owners = lax.dynamic_slice_in_dim(owners, first_page, pages, 0)
    before = jnp.arange(owners.shape[0], dtype=jnp.int32)[None, :] < (
        first_page + jnp.arange(pages, dtype=jnp.int32)
    )[:, None]
    same = owners[None, :] == my_owners[:, None]
    rank = jnp.sum((same & before).astype(jnp.int32), axis=1)
    onehot = my_owners[:, None] == jnp.arange(requests, dtype=jnp.int32)[None, :]
    start = jnp.sum(jnp.where(onehot, context_tokens[None, :], 0), axis=1)
    adapter = jnp.sum(jnp.where(onehot, request_adapter[None, :], 0), axis=1)
    near = NZH * NZM * NZP
    z = my_owners % near
    z_low = z % (NZM * NZP)
    owner_spot = ((my_owners // near) * (NZM * NZP) + z_low) * (2 * NZH) + z // (NZM * NZP)
    inside = jnp.arange(PAGE, dtype=jnp.int32)[None, :]
    position = ((start + rank * PAGE)[:, None] + inside).reshape(-1)
    token_adapter = jnp.broadcast_to(adapter[:, None], (pages, PAGE)).reshape(-1, 1)
    token_owner = jnp.broadcast_to(owner_spot[:, None], (pages, PAGE)).reshape(1, -1)
    half = HEAD // 2
    exponent = jnp.arange(half, dtype=f32) * (2.0 / HEAD)
    frequency = jnp.exp(-jnp.log(jnp.float32(rope_base)) * exponent)
    angles = position.astype(f32)[:, None] * frequency[None, :]
    cosine, sine = jnp.cos(angles), jnp.sin(angles)
    cosine = jnp.concatenate([cosine, cosine], axis=1)
    sine = jnp.concatenate([-sine, sine], axis=1)

    cache_o, cache_lse = cached_part(
        step_query[0],
        stored_keys[0],
        stored_values[0],
        jnp.sum(jnp.where(jnp.arange(requests) == device, context_tokens, 0)),
        step_key[0],
        step_value[0],
    )

    half_heads = heads // kv
    half_width = half_heads * HEAD
    full_width = half_width + HEAD
    members = NX * NZM * NZP
    unit = kv * NZH
    payload = pl.pallas_call(
        functools.partial(partial_kernel, half_heads, kv),
        in_specs=[SMEM] + [VMEM] * 10,
        out_specs=VMEM,
        out_shape=jax.ShapeDtypeStruct((members * unit, full_width), bf16),
        compiler_params=room(16),
        name="partial_attention",
    )(
        jnp.stack([me, parity]), base, from_partner, adapter_up_key, adapter_up_value,
        cosine, sine, token_adapter, token_owner, own_queries, pair_queries,
    )
    arrived = lax.all_to_all(payload.reshape(members, unit, full_width), NEAR, 0, 0, tiled=True)
    merged = pl.pallas_call(
        functools.partial(merge_near_kernel, half_heads),
        in_specs=[SMEM] + [VMEM] * 3,
        out_specs=VMEM,
        out_shape=jax.ShapeDtypeStruct((NZH * unit, full_width), bf16),
        compiler_params=room(12),
        name="merge_near",
    )(zh[None], arrived.reshape(members * unit, full_width), cache_o, cache_lse)
    across = lax.all_to_all(merged.reshape(NZH, unit, full_width), "zh", 0, 0, tiled=True)
    mixed = pl.pallas_call(
        functools.partial(merge_far_kernel, half_heads),
        in_specs=[VMEM],
        out_specs=VMEM,
        out_shape=jax.ShapeDtypeStruct((members * unit, half_width), bf16),
        compiler_params=room(12),
        name="merge_far",
    )(across.reshape(NZH * unit, full_width))
    rows = lax.all_to_all(mixed.reshape(members, unit, half_width), NEAR, 0, 0, tiled=True)
    pair = lax.axis_size("tp")
    columns = output_matrix.shape[1]
    partial_output = pl.pallas_call(
        output_kernel,
        in_specs=[VMEM] * 5,
        out_specs=VMEM,
        out_shape=jax.ShapeDtypeStruct((pair * columns, requests), f32),
        compiler_params=room(12),
        name="output_rows",
    )(
        rows.reshape(members * unit, half_width), output_matrix.T, adapter_down_output.T,
        adapter_up_output.T, request_adapter[None, :],
    )
    everything = lax.all_to_all(
        partial_output.reshape(pair, columns, requests), "tp", 0, 0, tiled=True
    )
    return jnp.sum(everything, axis=0).T.astype(bf16)


def solution(mesh):
    finer = Mesh(
        mesh.devices.reshape(mesh.shape["group"], NX, NZH, NZM, NZP, mesh.shape["tp"]),
        ("group", "x", "zh", "zm", "zp", "tp"),
    )
    placed = (
        P(GROUP_DEV, None),
        P(DEV, "tp"),
        P(DEV, "tp"),
        P(DEV, None),
        P(None, "tp"),
        P(None, "tp"),
        P("group"),
        P("group", None),
        P("group"),
        P(GROUP_DEV, "tp"),
        P(GROUP_DEV, "tp"),
        P(GROUP_DEV, "tp"),
        P(GROUP_DEV, None, "tp"),
        P(GROUP_DEV, None, "tp"),
        P("tp", DEV),
        P("tp", None),
        P(None, DEV),
    )
    return jax.shard_map(
        per_device, mesh=finer, in_specs=placed, out_specs=P("group", DEV), check_vma=False
    )
```

```python
import functools

import jax
import jax.numpy as jnp
from jax import lax
from jax.experimental import pallas as pl
from jax.experimental.pallas import tpu as pltpu
from jax.sharding import Mesh
from jax.sharding import PartitionSpec as P


HEADS = 32
KV_HEADS = 4
HEAD = 128
LOW_RANK = 16
ADAPTER_COUNT = 4
PAGE = 4
LORA = ADAPTER_COUNT * LOW_RANK
DEV = ("x", "zh", "zm", "zp")
GROUP_DEV = ("group", "x", "zh", "zm", "zp")
Z8 = ("zh", "zm")
NEAR = ("x", "zm", "zp")
NX, NZH, NZM, NZP = 8, 4, 2, 2
NEG = -1e30

rope_base = 500000.0


f32 = jnp.float32
bf16 = jnp.bfloat16
SMEM = pl.BlockSpec(memory_space=pltpu.SMEM)
VMEM = pl.BlockSpec(memory_space=pltpu.VMEM)


def room(mib):
    return pltpu.CompilerParams(vmem_limit_bytes=mib * 1024 * 1024)


def ring_x(x, step):
    return lax.ppermute(x, "x", [(i, (i + step) % NX) for i in range(NX)])


def swap_pair(x):
    return lax.ppermute(x, "zp", [(0, 1), (1, 0)])


def split_kernel(p_ref, a_ref, mine_ref, other_ref):
    half = HEAD // 2

    def write(even_ref, odd_ref):
        for k in range(even_ref.shape[1] // HEAD):
            t0 = a_ref[:, 2 * k * HEAD : (2 * k + 1) * HEAD]
            t1 = a_ref[:, (2 * k + 1) * HEAD : (2 * k + 2) * HEAD]
            cols = slice(k * HEAD, (k + 1) * HEAD)
            even_ref[:, cols] = jnp.concatenate([t0[:, :half], t1[:, :half]], axis=1)
            odd_ref[:, cols] = jnp.concatenate([t0[:, half:], t1[:, half:]], axis=1)

    @pl.when(p_ref[0] == 0)
    def _():
        write(mine_ref, other_ref)

    @pl.when(p_ref[0] != 0)
    def _():
        write(other_ref, mine_ref)


def split_columns(act, parity):
    rows, width = act.shape
    block = 32
    out = jax.ShapeDtypeStruct((rows, width // 2), bf16)
    return pl.pallas_call(
        split_kernel,
        grid=(rows // block,),
        in_specs=[SMEM, pl.BlockSpec((block, width), lambda i: (i, 0))],
        out_specs=[pl.BlockSpec((block, width // 2), lambda i: (i, 0))] * 2,
        out_shape=[out, out],
        compiler_params=room(58),
        name="split_columns",
    )(parity, act)


def project_kernel(offsets, chunks, depth, x_ref, a_ref, *refs):
    pieces, out_ref = refs[:-1], refs[-1]
    me = x_ref[0]
    total = None
    for i, off in enumerate(offsets):
        where = lax.rem(me + off, NX)
        start = pl.multiple_of(where * chunks * depth, chunks * depth)
        a = a_ref[:, pl.ds(start, chunks * depth)]
        w = jnp.concatenate(
            [pieces[i * chunks + c][0:depth, :] for c in range(chunks)], axis=0
        )
        part = jnp.dot(a, w, preferred_element_type=f32)
        total = part if total is None else total + part
    out_ref[...] = total.astype(out_ref.dtype)


def project(act, offsets, pieces, depth, me, dtype):
    chunks = len(pieces) // len(offsets)
    width = pieces[0].shape[1]
    return pl.pallas_call(
        functools.partial(project_kernel, offsets, chunks, depth),
        in_specs=[SMEM] + [VMEM] * (1 + len(pieces)),
        out_specs=VMEM,
        out_shape=jax.ShapeDtypeStruct((act.shape[0], width), dtype),
        compiler_params=room(20),
        name="project",
    )(me, act, *pieces)


def collect_kernel(after_ref, *refs):
    out_ref = refs[-1]
    rows, width = refs[0].shape[0], out_ref.shape[1]
    for j, ref in enumerate(refs[:-1]):
        out_ref[j * rows : (j + 1) * rows, :] = ref[:, :width]


def collect_tails(pieces, depth, width, after):
    rows = pieces[0].shape[0] - depth
    tail = pl.BlockSpec((rows, pieces[0].shape[1]), lambda i: (depth // rows, 0))
    total = rows * len(pieces)
    return pl.pallas_call(
        collect_kernel,
        grid=(1,),
        in_specs=[pl.BlockSpec(memory_space=pl.ANY)] + [tail] * len(pieces),
        out_specs=pl.BlockSpec((total, width), lambda i: (0, 0)),
        out_shape=jax.ShapeDtypeStruct((total, width), bf16),
        compiler_params=room(8),
        name="collect_tails",
    )(after, *pieces)


def two_terms(v):
    hi = v.astype(bf16)
    return hi, (v - hi.astype(f32)).astype(bf16)


def dot_fine(v, w):
    hi, lo = two_terms(v)
    return jnp.dot(hi, w, preferred_element_type=f32) + jnp.dot(lo, w, preferred_element_type=f32)


def three_terms(v):
    hi = v.astype(bf16).astype(f32)
    mid = (v - hi).astype(bf16).astype(f32)
    return hi, mid, v - hi - mid


def partial_kernel(
    heads, kv, s_ref, base_ref, other_ref, upk_ref, upv_ref, cos_ref, sin_ref,
    adapter_ref, owner_ref, q0_ref, q1_ref, out_ref,
):
    me, parity = s_ref[0], s_ref[1]
    tokens = base_ref.shape[0]
    rows = out_ref.shape[0]
    width = kv * HEAD
    raw = base_ref[...] + other_ref[...].astype(f32)
    column = lax.broadcasted_iota(jnp.int32, (tokens, 2 * LORA), 1)
    kept = lax.rem(column, LORA) // LOW_RANK == adapter_ref[...]
    chosen = jnp.where(kept, raw[:, 2 * width :], 0.0)
    key = raw[:, :width] + dot_fine(chosen[:, :LORA], upk_ref[...])
    value = (raw[:, width : 2 * width] + dot_fine(chosen[:, LORA:], upv_ref[...])).astype(bf16)
    turned = []
    for k in range(kv):
        part = key[:, k * HEAD : (k + 1) * HEAD]
        spun = part * cos_ref[...] + pltpu.roll(part, HEAD // 2, 1) * sin_ref[...]
        turned.append(spun.astype(bf16))
    source = q0_ref.shape[0]
    half_rows = rows // kv
    blocks = 4
    i = lax.broadcasted_iota(jnp.int32, (half_rows, source), 1)
    row = lax.broadcasted_iota(jnp.int32, (half_rows, source), 0)
    block = lax.rem(i, blocks)
    z8 = lax.rem(i // blocks, NZH * NZM)
    off = i // (blocks * NZH * NZM)
    xs = lax.rem(off + me, NX)
    spot = (xs * (NZM * NZP) + lax.rem(z8, NZM) * NZP) * NZH + z8 // NZM
    hit0 = row == spot + parity * NZH
    hit1 = row == spot + (1 - parity) * NZH
    mask = lax.broadcasted_iota(jnp.int32, (half_rows, tokens), 0) == owner_ref[...]
    lane = lax.broadcasted_iota(jnp.int32, (half_rows, HEAD), 1)
    across = (((1,), (1,)), ((), ()))
    outs = [[] for _ in range(kv)]
    for k in range(kv):
        stat = jnp.zeros((half_rows, HEAD), f32)
        for g in range(blocks // kv):
            right = block == k * (blocks // kv) + g
            pick0 = jnp.where(hit0 & right, 1.0, 0.0).astype(bf16)
            pick1 = jnp.where(hit1 & right, 1.0, 0.0).astype(bf16)
            got = jnp.dot(pick0, q0_ref[...], preferred_element_type=f32) + jnp.dot(
                pick1, q1_ref[...], preferred_element_type=f32
            )
            got = got.astype(bf16)
            for j in range(got.shape[1] // HEAD):
                h = g * (got.shape[1] // HEAD) + j
                q = got[:, j * HEAD : (j + 1) * HEAD]
                s = lax.dot_general(q, turned[k], across, preferred_element_type=f32)
                s = jnp.where(mask, s * (HEAD ** (-0.5)), NEG)
                top = jnp.max(s, axis=1, keepdims=True)
                e = jnp.where(mask, jnp.exp(s - top), 0.0)
                total = jnp.sum(e, axis=1, keepdims=True)
                o = jnp.dot(
                    e.astype(bf16), value[:, k * HEAD : (k + 1) * HEAD],
                    preferred_element_type=f32,
                )
                full = total > 0.0
                o = o * jnp.where(full, 1.0 / jnp.maximum(total, 1e-30), 0.0)
                outs[k].append(o.astype(bf16))
                lse = jnp.where(full, top + jnp.log(jnp.maximum(total, 1e-30)), NEG)
                hi, mid, lo = three_terms(lse)
                stat = jnp.where(lane == h, hi, stat)
                stat = jnp.where(lane == heads + h, mid, stat)
                stat = jnp.where(lane == 2 * heads + h, lo, stat)
        outs[k].append(stat.astype(bf16))
    to = lax.broadcasted_iota(jnp.int32, (rows, half_rows), 0)
    come = lax.broadcasted_iota(jnp.int32, (rows, half_rows), 1)
    unit = kv * NZH
    place = (come // NZH) * unit + lax.rem(come, NZH)
    moves = [
        jnp.where(to == place + k * NZH, 1.0, 0.0).astype(bf16) for k in range(kv)
    ]
    for h in range(heads + 1):
        moved = jnp.dot(moves[0], outs[0][h], preferred_element_type=f32)
        for k in range(1, kv):
            moved = moved + jnp.dot(moves[k], outs[k][h], preferred_element_type=f32)
        out_ref[:, h * HEAD : (h + 1) * HEAD] = moved.astype(bf16)


def reduce_rows(v, op):
    while v.shape[0] > 8:
        half = v.shape[0] // 2
        v = op(v[:half], v[half:])
    return v


def merge(heads, x_ref, cached, out_ref, with_stat):
    rows = x_ref.shape[0]
    copies = out_ref.shape[0] // 8
    st = x_ref[:, heads * HEAD :].astype(f32)
    lse = st + pltpu.roll(st, HEAD - heads, 1) + pltpu.roll(st, HEAD - 2 * heads, 1)
    lane = lax.broadcasted_iota(jnp.int32, (rows, HEAD), 1)
    lse = jnp.where(lane < heads, lse, 0.0)
    top = reduce_rows(lse, jnp.maximum)
    if cached is not None:
        zh, o_ref, lse_ref = cached
        row = lax.broadcasted_iota(jnp.int32, (8, HEAD), 0)
        first = row < NZH
        here = lax.rem(row, NZH) == zh
        cache_lse = jnp.where(first, lse_ref[0:1, :], lse_ref[1:2, :])
        top = jnp.where(here, jnp.maximum(top, cache_lse), top)
        cache_w = jnp.where(here, jnp.exp(cache_lse - top), 0.0)
    w = jnp.exp(lse - jnp.tile(top, (rows // 8, 1)))
    total = reduce_rows(w, jnp.add)
    if cached is not None:
        total = total + cache_w
    for h in range(heads):
        cols = slice(h * HEAD, (h + 1) * HEAD)
        o = reduce_rows(w[:, h : h + 1] * x_ref[:, cols].astype(f32), jnp.add)
        if cached is not None:
            kept = jnp.where(first, o_ref[0:1, cols], o_ref[1:2, cols])
            o = o + cache_w[:, h : h + 1] * kept
        o = (o / total[:, h : h + 1]).astype(bf16)
        for c in range(copies):
            out_ref[c * 8 : (c + 1) * 8, cols] = o
    if with_stat:
        final = top + jnp.log(total)
        hi, mid, lo = three_terms(jnp.where(lane[:8] < heads, final, 0.0))
        stat = hi + pltpu.roll(mid, heads, 1) + pltpu.roll(lo, 2 * heads, 1)
        for c in range(copies):
            out_ref[c * 8 : (c + 1) * 8, heads * HEAD :] = stat.astype(bf16)


def merge_near_kernel(heads, s_ref, x_ref, o_ref, lse_ref, out_ref):
    merge(heads, x_ref, (s_ref[0], o_ref, lse_ref), out_ref, True)


def merge_far_kernel(heads, x_ref, out_ref):
    merge(heads, x_ref, None, out_ref, False)


def output_kernel(x_ref, w_ref, down_ref, up_ref, adapter_ref, out_ref):
    rows = adapter_ref.shape[1]
    half_width = x_ref.shape[1]
    i = lax.broadcasted_iota(jnp.int32, (rows, x_ref.shape[0]), 1)
    r = lax.broadcasted_iota(jnp.int32, (rows, x_ref.shape[0]), 0)
    near = NZM * NZP
    member = i // (2 * NZH)
    hit = r == (member // near) * (near * NZH) + lax.rem(i, NZH) * near + lax.rem(member, near)
    half = lax.rem(i // NZH, 2)
    across = (((1,), (1,)), ((), ()))
    plain = jnp.zeros((w_ref.shape[0], rows), f32)
    narrow = jnp.zeros((down_ref.shape[0], rows), f32)
    for k in range(2):
        pick = jnp.where(hit & (half == k), 1.0, 0.0).astype(bf16)
        x = jnp.dot(pick, x_ref[...], preferred_element_type=f32).astype(bf16)
        cols = slice(k * half_width, (k + 1) * half_width)
        plain = plain + lax.dot_general(w_ref[:, cols], x, across, preferred_element_type=f32)
        narrow = narrow + lax.dot_general(down_ref[:, cols], x, across, preferred_element_type=f32)
    column = lax.broadcasted_iota(jnp.int32, narrow.shape, 0)
    hi, lo = two_terms(jnp.where(column // LOW_RANK == adapter_ref[...], narrow, 0.0))
    up = up_ref[...]
    plain = plain + (
        jnp.dot(up, hi, preferred_element_type=f32) + jnp.dot(up, lo, preferred_element_type=f32)
    )
    count = w_ref.shape[0]
    for c in range(out_ref.shape[0] // count):
        out_ref[c * count : (c + 1) * count, :] = plain


def cached_part(query, old_keys, old_values, old_length, last_key, last_value):
    group = HEADS // KV_HEADS
    q = query.reshape(-1, group, HEAD)
    kv = q.shape[0]
    scale = HEAD ** (-0.5)

    def score_of(keys):
        shaped = keys.reshape(keys.shape[0], kv, HEAD)
        return jnp.einsum("kgd,lkd->kgl", q, shaped, preferred_element_type=f32) * scale

    def mix_with(weights, values):
        shaped = values.reshape(values.shape[0], kv, HEAD)
        return jnp.einsum("kgl,lkd->kgd", weights, shaped, preferred_element_type=f32)

    valid = jnp.arange(old_keys.shape[0], dtype=jnp.int32) < old_length
    old = jnp.where(valid[None, None, :], score_of(old_keys), NEG)
    last = score_of(last_key[None, :])
    top = jnp.maximum(jnp.max(old, axis=-1, keepdims=True), last)
    old_w = jnp.exp(old - top)
    last_w = jnp.exp(last - top)
    total = jnp.sum(old_w, axis=-1, keepdims=True) + last_w
    o = mix_with((old_w / total).astype(bf16), old_values)
    o = o + mix_with((last_w / total).astype(bf16), last_value[None, :])
    lse = (top + jnp.log(total)).reshape(kv, -1)
    return o.reshape(kv, -1), jnp.pad(lse, ((0, 0), (0, HEAD - lse.shape[1])))


def per_device(
    prompt_activations,
    key_matrix,
    value_matrix,
    adapter_down_keyvalue,
    adapter_up_key,
    adapter_up_value,
    request_adapter,
    page_request,
    context_tokens,
    step_query,
    step_key,
    step_value,
    stored_keys,
    stored_values,
    output_matrix,
    adapter_down_output,
    adapter_up_output,
):
    device = lax.axis_index(DEV)
    me = lax.axis_index("x").astype(jnp.int32)
    parity = lax.axis_index("zp").astype(jnp.int32)
    zh = lax.axis_index("zh").astype(jnp.int32)
    tokens = prompt_activations.shape[0]
    pages = tokens // PAGE
    requests = request_adapter.shape[0]
    kv = key_matrix.shape[1] // HEAD
    heads = step_query.shape[1] // HEAD
    depth = key_matrix.shape[0]
    width = 2 * key_matrix.shape[1] + adapter_down_keyvalue.shape[1]

    weights = jnp.concatenate([key_matrix, value_matrix, adapter_down_keyvalue], axis=1)
    query_rows = jnp.pad(step_query.reshape(4, -1), ((0, 4), (0, width - step_query.shape[1] // 4)))
    block = jnp.concatenate([weights, query_rows], axis=0)
    column = lax.all_gather(block, Z8)
    count = column.shape[0]
    chunks = 2
    per_chunk = count // chunks
    pieces = []
    for c in range(chunks):
        part = column[c * per_chunk : (c + 1) * per_chunk]
        pieces.append(
            jnp.concatenate(
                [
                    part[:, :depth].reshape(per_chunk * depth, width),
                    part[:, depth : depth + 4].reshape(per_chunk * 4, width),
                ],
                axis=0,
            )
        )
    chunk_depth = per_chunk * depth

    mine, theirs = split_columns(prompt_activations, parity[None])
    partner_act = swap_pair(theirs)

    by_offset = {0: pieces}
    ahead = behind = pieces
    for s in range(1, NX // 2):
        ahead = [ring_x(a, 1) for a in ahead]
        behind = [ring_x(b, -1) for b in behind]
        by_offset[NX - s] = ahead
        by_offset[s] = behind
    by_offset[NX // 2] = [ring_x(ahead[0], 1), ring_x(behind[1], -1)]
    offsets = (0, 7, 1, 6, 2, 5, 3, 4)
    flat = [a for off in range(NX) for a in by_offset[off]]
    ordered = [a for off in offsets for a in by_offset[off]]

    quarter = step_query.shape[1] // 4
    partial_other = project(partner_act, offsets, ordered, chunk_depth, me[None], bf16)
    from_partner = swap_pair(partial_other)
    own_queries = collect_tails(flat, chunk_depth, quarter, partial_other)
    pair_queries = swap_pair(own_queries)
    base = project(mine, offsets, ordered, chunk_depth, me[None], f32)

    owners = page_request[:, 0]
    first_page = device * pages
    my_owners = lax.dynamic_slice_in_dim(owners, first_page, pages, 0)
    before = jnp.arange(owners.shape[0], dtype=jnp.int32)[None, :] < (
        first_page + jnp.arange(pages, dtype=jnp.int32)
    )[:, None]
    same = owners[None, :] == my_owners[:, None]
    rank = jnp.sum((same & before).astype(jnp.int32), axis=1)
    onehot = my_owners[:, None] == jnp.arange(requests, dtype=jnp.int32)[None, :]
    start = jnp.sum(jnp.where(onehot, context_tokens[None, :], 0), axis=1)
    adapter = jnp.sum(jnp.where(onehot, request_adapter[None, :], 0), axis=1)
    near = NZH * NZM * NZP
    z = my_owners % near
    z_low = z % (NZM * NZP)
    owner_spot = ((my_owners // near) * (NZM * NZP) + z_low) * NZH + z // (NZM * NZP)
    inside = jnp.arange(PAGE, dtype=jnp.int32)[None, :]
    position = ((start + rank * PAGE)[:, None] + inside).reshape(-1)
    token_adapter = jnp.broadcast_to(adapter[:, None], (pages, PAGE)).reshape(-1, 1)
    token_owner = jnp.broadcast_to(owner_spot[:, None], (pages, PAGE)).reshape(1, -1)
    half = HEAD // 2
    exponent = jnp.arange(half, dtype=f32) * (2.0 / HEAD)
    frequency = jnp.exp(-jnp.log(jnp.float32(rope_base)) * exponent)
    angles = position.astype(f32)[:, None] * frequency[None, :]
    cosine, sine = jnp.cos(angles), jnp.sin(angles)
    cosine = jnp.concatenate([cosine, cosine], axis=1)
    sine = jnp.concatenate([-sine, sine], axis=1)

    cache_o, cache_lse = cached_part(
        step_query[0],
        stored_keys[0],
        stored_values[0],
        jnp.sum(jnp.where(jnp.arange(requests) == device, context_tokens, 0)),
        step_key[0],
        step_value[0],
    )

    half_heads = heads // kv
    half_width = half_heads * HEAD
    full_width = half_width + HEAD
    members = NX * NZM * NZP
    unit = kv * NZH
    payload = pl.pallas_call(
        functools.partial(partial_kernel, half_heads, kv),
        in_specs=[SMEM] + [VMEM] * 10,
        out_specs=VMEM,
        out_shape=jax.ShapeDtypeStruct((members * unit, full_width), bf16),
        compiler_params=room(16),
        name="partial_attention",
    )(
        jnp.stack([me, parity]), base, from_partner, adapter_up_key, adapter_up_value,
        cosine, sine, token_adapter, token_owner, own_queries, pair_queries,
    )
    arrived = lax.all_to_all(payload.reshape(members, unit, full_width), NEAR, 0, 0, tiled=True)
    merged = pl.pallas_call(
        functools.partial(merge_near_kernel, half_heads),
        in_specs=[SMEM] + [VMEM] * 3,
        out_specs=VMEM,
        out_shape=jax.ShapeDtypeStruct((NZH * unit, full_width), bf16),
        compiler_params=room(12),
        name="merge_near",
    )(zh[None], arrived.reshape(members * unit, full_width), cache_o, cache_lse)
    across = lax.all_to_all(merged.reshape(NZH, unit, full_width), "zh", 0, 0, tiled=True)
    mixed = pl.pallas_call(
        functools.partial(merge_far_kernel, half_heads),
        in_specs=[VMEM],
        out_specs=VMEM,
        out_shape=jax.ShapeDtypeStruct((members * unit, half_width), bf16),
        compiler_params=room(12),
        name="merge_far",
    )(across.reshape(NZH * unit, full_width))
    rows = lax.all_to_all(mixed.reshape(members, unit, half_width), NEAR, 0, 0, tiled=True)
    pair = lax.axis_size("tp")
    columns = output_matrix.shape[1]
    partial_output = pl.pallas_call(
        output_kernel,
        in_specs=[VMEM] * 5,
        out_specs=VMEM,
        out_shape=jax.ShapeDtypeStruct((pair * columns, requests), f32),
        compiler_params=room(12),
        name="output_rows",
    )(
        rows.reshape(members * unit, half_width), output_matrix.T, adapter_down_output.T,
        adapter_up_output.T, request_adapter[None, :],
    )
    everything = lax.all_to_all(
        partial_output.reshape(pair, columns, requests), "tp", 0, 0, tiled=True
    )
    return jnp.sum(everything, axis=0).T.astype(bf16)


def solution(mesh):
    finer = Mesh(
        mesh.devices.reshape(mesh.shape["group"], NX, NZH, NZM, NZP, mesh.shape["tp"]),
        ("group", "x", "zh", "zm", "zp", "tp"),
    )
    placed = (
        P(GROUP_DEV, None),
        P(DEV, "tp"),
        P(DEV, "tp"),
        P(DEV, None),
        P(None, "tp"),
        P(None, "tp"),
        P("group"),
        P("group", None),
        P("group"),
        P(GROUP_DEV, "tp"),
        P(GROUP_DEV, "tp"),
        P(GROUP_DEV, "tp"),
        P(GROUP_DEV, None, "tp"),
        P(GROUP_DEV, None, "tp"),
        P("tp", DEV),
        P("tp", None),
        P(None, DEV),
    )
    return jax.shard_map(
        per_device, mesh=finer, in_specs=placed, out_specs=P("group", DEV), check_vma=False
    )
```

```python
import functools

import jax
import jax.numpy as jnp
from jax import lax
from jax.experimental import pallas as pl
from jax.experimental.pallas import tpu as pltpu
from jax.sharding import Mesh
from jax.sharding import PartitionSpec as P


HEADS = 32
KV_HEADS = 4
HEAD = 128
LOW_RANK = 16
ADAPTER_COUNT = 4
PAGE = 4
LORA = ADAPTER_COUNT * LOW_RANK
DEV = ("x", "zh", "zm", "zp")
GROUP_DEV = ("group", "x", "zh", "zm", "zp")
Z8 = ("zh", "zm")
NEAR = ("x", "zm", "zp")
NX, NZH, NZM, NZP = 8, 4, 2, 2
NEG = -1e30

rope_base = 500000.0


f32 = jnp.float32
bf16 = jnp.bfloat16
SMEM = pl.BlockSpec(memory_space=pltpu.SMEM)
VMEM = pl.BlockSpec(memory_space=pltpu.VMEM)


def room(mib):
    return pltpu.CompilerParams(vmem_limit_bytes=mib * 1024 * 1024)


def ring_x(x, step):
    return lax.ppermute(x, "x", [(i, (i + step) % NX) for i in range(NX)])


def swap_pair(x):
    return lax.ppermute(x, "zp", [(0, 1), (1, 0)])


def select_kernel(p_ref, a_ref, out_ref):
    half = HEAD // 2

    def write(at):
        for k in range(out_ref.shape[1] // HEAD):
            t0 = a_ref[:, 2 * k * HEAD + at : 2 * k * HEAD + at + half]
            t1 = a_ref[:, (2 * k + 1) * HEAD + at : (2 * k + 1) * HEAD + at + half]
            out_ref[:, k * HEAD : (k + 1) * HEAD] = jnp.concatenate([t0, t1], axis=1)

    @pl.when(p_ref[0] == 0)
    def _():
        write(0)

    @pl.when(p_ref[0] != 0)
    def _():
        write(half)


def select_columns(act, parity, mib):
    rows, width = act.shape
    block = 32
    return pl.pallas_call(
        select_kernel,
        grid=(rows // block,),
        in_specs=[SMEM, pl.BlockSpec((block, width), lambda i: (i, 0))],
        out_specs=pl.BlockSpec((block, width // 2), lambda i: (i, 0)),
        out_shape=jax.ShapeDtypeStruct((rows, width // 2), bf16),
        compiler_params=room(mib),
        name="select_columns",
    )(parity, act)


def project_kernel(offsets, chunks, depth, x_ref, a_ref, *refs):
    pieces, out_ref = refs[:-1], refs[-1]
    me = x_ref[0]
    total = None
    for i, off in enumerate(offsets):
        where = lax.rem(me + off, NX)
        start = pl.multiple_of(where * chunks * depth, chunks * depth)
        a = a_ref[:, pl.ds(start, chunks * depth)]
        w = jnp.concatenate(
            [pieces[i * chunks + c][0:depth, :] for c in range(chunks)], axis=0
        )
        part = jnp.dot(a, w, preferred_element_type=f32)
        total = part if total is None else total + part
    out_ref[...] = total.astype(out_ref.dtype)


def project(act, offsets, pieces, depth, me, dtype):
    chunks = len(pieces) // len(offsets)
    width = pieces[0].shape[1]
    return pl.pallas_call(
        functools.partial(project_kernel, offsets, chunks, depth),
        in_specs=[SMEM] + [VMEM] * (1 + len(pieces)),
        out_specs=VMEM,
        out_shape=jax.ShapeDtypeStruct((act.shape[0], width), dtype),
        compiler_params=room(20),
        name="project",
    )(me, act, *pieces)


def collect_kernel(after_ref, *refs):
    out_ref = refs[-1]
    rows, width = refs[0].shape[0], out_ref.shape[1]
    for j, ref in enumerate(refs[:-1]):
        out_ref[j * rows : (j + 1) * rows, :] = ref[:, :width]


def collect_tails(pieces, depth, width, after):
    rows = pieces[0].shape[0] - depth
    tail = pl.BlockSpec((rows, pieces[0].shape[1]), lambda i: (depth // rows, 0))
    total = rows * len(pieces)
    return pl.pallas_call(
        collect_kernel,
        grid=(1,),
        in_specs=[pl.BlockSpec(memory_space=pl.ANY)] + [tail] * len(pieces),
        out_specs=pl.BlockSpec((total, width), lambda i: (0, 0)),
        out_shape=jax.ShapeDtypeStruct((total, width), bf16),
        compiler_params=room(8),
        name="collect_tails",
    )(after, *pieces)


def two_terms(v):
    hi = v.astype(bf16)
    return hi, (v - hi.astype(f32)).astype(bf16)


def dot_fine(v, w):
    hi, lo = two_terms(v)
    return jnp.dot(hi, w, preferred_element_type=f32) + jnp.dot(lo, w, preferred_element_type=f32)


def three_terms(v):
    hi = v.astype(bf16).astype(f32)
    mid = (v - hi).astype(bf16).astype(f32)
    return hi, mid, v - hi - mid


def partial_kernel(
    heads, kv, s_ref, base_ref, other_ref, upk_ref, upv_ref, cos_ref, sin_ref,
    adapter_ref, owner_ref, q0_ref, q1_ref, out_ref,
):
    me, parity = s_ref[0], s_ref[1]
    tokens = base_ref.shape[0]
    rows = out_ref.shape[0]
    width = kv * HEAD
    raw = base_ref[...] + other_ref[...].astype(f32)
    column = lax.broadcasted_iota(jnp.int32, (tokens, 2 * LORA), 1)
    kept = lax.rem(column, LORA) // LOW_RANK == adapter_ref[...]
    chosen = jnp.where(kept, raw[:, 2 * width :], 0.0)
    key = raw[:, :width] + dot_fine(chosen[:, :LORA], upk_ref[...])
    value = (raw[:, width : 2 * width] + dot_fine(chosen[:, LORA:], upv_ref[...])).astype(bf16)
    turned = []
    for k in range(kv):
        part = key[:, k * HEAD : (k + 1) * HEAD]
        spun = part * cos_ref[...] + pltpu.roll(part, HEAD // 2, 1) * sin_ref[...]
        turned.append(spun.astype(bf16))
    source = q0_ref.shape[0]
    half_rows = rows // kv
    blocks = 4
    i = lax.broadcasted_iota(jnp.int32, (half_rows, source), 1)
    row = lax.broadcasted_iota(jnp.int32, (half_rows, source), 0)
    block = lax.rem(i, blocks)
    z8 = lax.rem(i // blocks, NZH * NZM)
    off = i // (blocks * NZH * NZM)
    xs = lax.rem(off + me, NX)
    spot = (xs * (NZM * NZP) + lax.rem(z8, NZM) * NZP) * NZH + z8 // NZM
    hit0 = row == spot + parity * NZH
    hit1 = row == spot + (1 - parity) * NZH
    mask = lax.broadcasted_iota(jnp.int32, (half_rows, tokens), 0) == owner_ref[...]
    lane = lax.broadcasted_iota(jnp.int32, (half_rows, HEAD), 1)
    across = (((1,), (1,)), ((), ()))
    outs = [[] for _ in range(kv)]
    for k in range(kv):
        stat = jnp.zeros((half_rows, HEAD), f32)
        for g in range(blocks // kv):
            right = block == k * (blocks // kv) + g
            pick0 = jnp.where(hit0 & right, 1.0, 0.0).astype(bf16)
            pick1 = jnp.where(hit1 & right, 1.0, 0.0).astype(bf16)
            got = jnp.dot(pick0, q0_ref[...], preferred_element_type=f32) + jnp.dot(
                pick1, q1_ref[...], preferred_element_type=f32
            )
            got = got.astype(bf16)
            for j in range(got.shape[1] // HEAD):
                h = g * (got.shape[1] // HEAD) + j
                q = got[:, j * HEAD : (j + 1) * HEAD]
                s = lax.dot_general(q, turned[k], across, preferred_element_type=f32)
                s = jnp.where(mask, s * (HEAD ** (-0.5)), NEG)
                top = jnp.max(s, axis=1, keepdims=True)
                e = jnp.where(mask, jnp.exp(s - top), 0.0)
                total = jnp.sum(e, axis=1, keepdims=True)
                o = jnp.dot(
                    e.astype(bf16), value[:, k * HEAD : (k + 1) * HEAD],
                    preferred_element_type=f32,
                )
                full = total > 0.0
                o = o * jnp.where(full, 1.0 / jnp.maximum(total, 1e-30), 0.0)
                outs[k].append(o.astype(bf16))
                lse = jnp.where(full, top + jnp.log(jnp.maximum(total, 1e-30)), NEG)
                hi, mid, lo = three_terms(lse)
                stat = jnp.where(lane == h, hi, stat)
                stat = jnp.where(lane == heads + h, mid, stat)
                stat = jnp.where(lane == 2 * heads + h, lo, stat)
        outs[k].append(stat.astype(bf16))
    to = lax.broadcasted_iota(jnp.int32, (rows, half_rows), 0)
    come = lax.broadcasted_iota(jnp.int32, (rows, half_rows), 1)
    unit = kv * NZH
    place = (come // NZH) * unit + lax.rem(come, NZH)
    moves = [
        jnp.where(to == place + k * NZH, 1.0, 0.0).astype(bf16) for k in range(kv)
    ]
    for h in range(heads + 1):
        moved = jnp.dot(moves[0], outs[0][h], preferred_element_type=f32)
        for k in range(1, kv):
            moved = moved + jnp.dot(moves[k], outs[k][h], preferred_element_type=f32)
        out_ref[:, h * HEAD : (h + 1) * HEAD] = moved.astype(bf16)


def reduce_rows(v, op):
    while v.shape[0] > 8:
        half = v.shape[0] // 2
        v = op(v[:half], v[half:])
    return v


def merge(heads, x_ref, cached, out_ref, with_stat):
    rows = x_ref.shape[0]
    copies = out_ref.shape[0] // 8
    st = x_ref[:, heads * HEAD :].astype(f32)
    lse = st + pltpu.roll(st, HEAD - heads, 1) + pltpu.roll(st, HEAD - 2 * heads, 1)
    lane = lax.broadcasted_iota(jnp.int32, (rows, HEAD), 1)
    lse = jnp.where(lane < heads, lse, 0.0)
    top = reduce_rows(lse, jnp.maximum)
    if cached is not None:
        zh, o_ref, lse_ref = cached
        row = lax.broadcasted_iota(jnp.int32, (8, HEAD), 0)
        first = row < NZH
        here = lax.rem(row, NZH) == zh
        cache_lse = jnp.where(first, lse_ref[0:1, :], lse_ref[1:2, :])
        top = jnp.where(here, jnp.maximum(top, cache_lse), top)
        cache_w = jnp.where(here, jnp.exp(cache_lse - top), 0.0)
    w = jnp.exp(lse - jnp.tile(top, (rows // 8, 1)))
    total = reduce_rows(w, jnp.add)
    if cached is not None:
        total = total + cache_w
    for h in range(heads):
        cols = slice(h * HEAD, (h + 1) * HEAD)
        o = reduce_rows(w[:, h : h + 1] * x_ref[:, cols].astype(f32), jnp.add)
        if cached is not None:
            kept = jnp.where(first, o_ref[0:1, cols], o_ref[1:2, cols])
            o = o + cache_w[:, h : h + 1] * kept
        o = (o / total[:, h : h + 1]).astype(bf16)
        for c in range(copies):
            out_ref[c * 8 : (c + 1) * 8, cols] = o
    if with_stat:
        final = top + jnp.log(total)
        hi, mid, lo = three_terms(jnp.where(lane[:8] < heads, final, 0.0))
        stat = hi + pltpu.roll(mid, heads, 1) + pltpu.roll(lo, 2 * heads, 1)
        for c in range(copies):
            out_ref[c * 8 : (c + 1) * 8, heads * HEAD :] = stat.astype(bf16)


def merge_near_kernel(heads, s_ref, x_ref, o_ref, lse_ref, out_ref):
    merge(heads, x_ref, (s_ref[0], o_ref, lse_ref), out_ref, True)


def merge_far_kernel(heads, x_ref, out_ref):
    merge(heads, x_ref, None, out_ref, False)


def output_kernel(x_ref, w_ref, down_ref, up_ref, adapter_ref, out_ref):
    rows = adapter_ref.shape[1]
    half_width = x_ref.shape[1]
    i = lax.broadcasted_iota(jnp.int32, (rows, x_ref.shape[0]), 1)
    r = lax.broadcasted_iota(jnp.int32, (rows, x_ref.shape[0]), 0)
    near = NZM * NZP
    member = i // (2 * NZH)
    hit = r == (member // near) * (near * NZH) + lax.rem(i, NZH) * near + lax.rem(member, near)
    half = lax.rem(i // NZH, 2)
    across = (((1,), (1,)), ((), ()))
    plain = jnp.zeros((w_ref.shape[0], rows), f32)
    narrow = jnp.zeros((down_ref.shape[0], rows), f32)
    for k in range(2):
        pick = jnp.where(hit & (half == k), 1.0, 0.0).astype(bf16)
        x = jnp.dot(pick, x_ref[...], preferred_element_type=f32).astype(bf16)
        cols = slice(k * half_width, (k + 1) * half_width)
        plain = plain + lax.dot_general(w_ref[:, cols], x, across, preferred_element_type=f32)
        narrow = narrow + lax.dot_general(down_ref[:, cols], x, across, preferred_element_type=f32)
    column = lax.broadcasted_iota(jnp.int32, narrow.shape, 0)
    hi, lo = two_terms(jnp.where(column // LOW_RANK == adapter_ref[...], narrow, 0.0))
    up = up_ref[...]
    plain = plain + (
        jnp.dot(up, hi, preferred_element_type=f32) + jnp.dot(up, lo, preferred_element_type=f32)
    )
    count = w_ref.shape[0]
    for c in range(out_ref.shape[0] // count):
        out_ref[c * count : (c + 1) * count, :] = plain


def cached_part(query, old_keys, old_values, old_length, last_key, last_value):
    group = HEADS // KV_HEADS
    q = query.reshape(-1, group, HEAD)
    kv = q.shape[0]
    scale = HEAD ** (-0.5)

    def score_of(keys):
        shaped = keys.reshape(keys.shape[0], kv, HEAD)
        return jnp.einsum("kgd,lkd->kgl", q, shaped, preferred_element_type=f32) * scale

    def mix_with(weights, values):
        shaped = values.reshape(values.shape[0], kv, HEAD)
        return jnp.einsum("kgl,lkd->kgd", weights, shaped, preferred_element_type=f32)

    valid = jnp.arange(old_keys.shape[0], dtype=jnp.int32) < old_length
    old = jnp.where(valid[None, None, :], score_of(old_keys), NEG)
    last = score_of(last_key[None, :])
    top = jnp.maximum(jnp.max(old, axis=-1, keepdims=True), last)
    old_w = jnp.exp(old - top)
    last_w = jnp.exp(last - top)
    total = jnp.sum(old_w, axis=-1, keepdims=True) + last_w
    o = mix_with((old_w / total).astype(bf16), old_values)
    o = o + mix_with((last_w / total).astype(bf16), last_value[None, :])
    lse = (top + jnp.log(total)).reshape(kv, -1)
    return o.reshape(kv, -1), jnp.pad(lse, ((0, 0), (0, HEAD - lse.shape[1])))


def per_device(
    prompt_activations,
    key_matrix,
    value_matrix,
    adapter_down_keyvalue,
    adapter_up_key,
    adapter_up_value,
    request_adapter,
    page_request,
    context_tokens,
    step_query,
    step_key,
    step_value,
    stored_keys,
    stored_values,
    output_matrix,
    adapter_down_output,
    adapter_up_output,
):
    device = lax.axis_index(DEV)
    me = lax.axis_index("x").astype(jnp.int32)
    parity = lax.axis_index("zp").astype(jnp.int32)
    zh = lax.axis_index("zh").astype(jnp.int32)
    tokens = prompt_activations.shape[0]
    pages = tokens // PAGE
    requests = request_adapter.shape[0]
    kv = key_matrix.shape[1] // HEAD
    heads = step_query.shape[1] // HEAD
    depth = key_matrix.shape[0]
    width = 2 * key_matrix.shape[1] + adapter_down_keyvalue.shape[1]

    weights = jnp.concatenate([key_matrix, value_matrix, adapter_down_keyvalue], axis=1)
    query_rows = jnp.pad(step_query.reshape(4, -1), ((0, 4), (0, width - step_query.shape[1] // 4)))
    block = jnp.concatenate([weights, query_rows], axis=0)
    column = lax.all_gather(block, Z8)
    count = column.shape[0]
    chunks = 2
    per_chunk = count // chunks
    pieces = []
    for c in range(chunks):
        part = column[c * per_chunk : (c + 1) * per_chunk]
        pieces.append(
            jnp.concatenate(
                [
                    part[:, :depth].reshape(per_chunk * depth, width),
                    part[:, depth : depth + 4].reshape(per_chunk * 4, width),
                ],
                axis=0,
            )
        )
    chunk_depth = per_chunk * depth

    theirs = select_columns(prompt_activations, 1 - parity[None], 58)
    mine = select_columns(prompt_activations, parity[None], 50)
    partner_act = swap_pair(theirs)

    by_offset = {0: pieces}
    ahead = behind = pieces
    for s in range(1, NX // 2):
        ahead = [ring_x(a, 1) for a in ahead]
        behind = [ring_x(b, -1) for b in behind]
        by_offset[NX - s] = ahead
        by_offset[s] = behind
    by_offset[NX // 2] = [ring_x(ahead[0], 1), ring_x(behind[1], -1)]
    offsets = (0, 7, 1, 6, 2, 5, 3, 4)
    flat = [a for off in range(NX) for a in by_offset[off]]
    ordered = [a for off in offsets for a in by_offset[off]]

    quarter = step_query.shape[1] // 4
    partial_other = project(partner_act, offsets, ordered, chunk_depth, me[None], bf16)
    from_partner = swap_pair(partial_other)
    own_queries = collect_tails(flat, chunk_depth, quarter, partial_other)
    pair_queries = swap_pair(own_queries)
    base = project(mine, offsets, ordered, chunk_depth, me[None], f32)

    owners = page_request[:, 0]
    first_page = device * pages
    my_owners = lax.dynamic_slice_in_dim(owners, first_page, pages, 0)
    before = jnp.arange(owners.shape[0], dtype=jnp.int32)[None, :] < (
        first_page + jnp.arange(pages, dtype=jnp.int32)
    )[:, None]
    same = owners[None, :] == my_owners[:, None]
    rank = jnp.sum((same & before).astype(jnp.int32), axis=1)
    onehot = my_owners[:, None] == jnp.arange(requests, dtype=jnp.int32)[None, :]
    start = jnp.sum(jnp.where(onehot, context_tokens[None, :], 0), axis=1)
    adapter = jnp.sum(jnp.where(onehot, request_adapter[None, :], 0), axis=1)
    near = NZH * NZM * NZP
    z = my_owners % near
    z_low = z % (NZM * NZP)
    owner_spot = ((my_owners // near) * (NZM * NZP) + z_low) * NZH + z // (NZM * NZP)
    inside = jnp.arange(PAGE, dtype=jnp.int32)[None, :]
    position = ((start + rank * PAGE)[:, None] + inside).reshape(-1)
    token_adapter = jnp.broadcast_to(adapter[:, None], (pages, PAGE)).reshape(-1, 1)
    token_owner = jnp.broadcast_to(owner_spot[:, None], (pages, PAGE)).reshape(1, -1)
    half = HEAD // 2
    exponent = jnp.arange(half, dtype=f32) * (2.0 / HEAD)
    frequency = jnp.exp(-jnp.log(jnp.float32(rope_base)) * exponent)
    angles = position.astype(f32)[:, None] * frequency[None, :]
    cosine, sine = jnp.cos(angles), jnp.sin(angles)
    cosine = jnp.concatenate([cosine, cosine], axis=1)
    sine = jnp.concatenate([-sine, sine], axis=1)

    cache_o, cache_lse = cached_part(
        step_query[0],
        stored_keys[0],
        stored_values[0],
        jnp.sum(jnp.where(jnp.arange(requests) == device, context_tokens, 0)),
        step_key[0],
        step_value[0],
    )

    half_heads = heads // kv
    half_width = half_heads * HEAD
    full_width = half_width + HEAD
    members = NX * NZM * NZP
    unit = kv * NZH
    payload = pl.pallas_call(
        functools.partial(partial_kernel, half_heads, kv),
        in_specs=[SMEM] + [VMEM] * 10,
        out_specs=VMEM,
        out_shape=jax.ShapeDtypeStruct((members * unit, full_width), bf16),
        compiler_params=room(16),
        name="partial_attention",
    )(
        jnp.stack([me, parity]), base, from_partner, adapter_up_key, adapter_up_value,
        cosine, sine, token_adapter, token_owner, own_queries, pair_queries,
    )
    arrived = lax.all_to_all(payload.reshape(members, unit, full_width), NEAR, 0, 0, tiled=True)
    merged = pl.pallas_call(
        functools.partial(merge_near_kernel, half_heads),
        in_specs=[SMEM] + [VMEM] * 3,
        out_specs=VMEM,
        out_shape=jax.ShapeDtypeStruct((NZH * unit, full_width), bf16),
        compiler_params=room(12),
        name="merge_near",
    )(zh[None], arrived.reshape(members * unit, full_width), cache_o, cache_lse)
    across = lax.all_to_all(merged.reshape(NZH, unit, full_width), "zh", 0, 0, tiled=True)
    mixed = pl.pallas_call(
        functools.partial(merge_far_kernel, half_heads),
        in_specs=[VMEM],
        out_specs=VMEM,
        out_shape=jax.ShapeDtypeStruct((members * unit, half_width), bf16),
        compiler_params=room(12),
        name="merge_far",
    )(across.reshape(NZH * unit, full_width))
    rows = lax.all_to_all(mixed.reshape(members, unit, half_width), NEAR, 0, 0, tiled=True)
    pair = lax.axis_size("tp")
    columns = output_matrix.shape[1]
    partial_output = pl.pallas_call(
        output_kernel,
        in_specs=[VMEM] * 5,
        out_specs=VMEM,
        out_shape=jax.ShapeDtypeStruct((pair * columns, requests), f32),
        compiler_params=room(12),
        name="output_rows",
    )(
        rows.reshape(members * unit, half_width), output_matrix.T, adapter_down_output.T,
        adapter_up_output.T, request_adapter[None, :],
    )
    everything = lax.all_to_all(
        partial_output.reshape(pair, columns, requests), "tp", 0, 0, tiled=True
    )
    return jnp.sum(everything, axis=0).T.astype(bf16)


def solution(mesh):
    finer = Mesh(
        mesh.devices.reshape(mesh.shape["group"], NX, NZH, NZM, NZP, mesh.shape["tp"]),
        ("group", "x", "zh", "zm", "zp", "tp"),
    )
    placed = (
        P(GROUP_DEV, None),
        P(DEV, "tp"),
        P(DEV, "tp"),
        P(DEV, None),
        P(None, "tp"),
        P(None, "tp"),
        P("group"),
        P("group", None),
        P("group"),
        P(GROUP_DEV, "tp"),
        P(GROUP_DEV, "tp"),
        P(GROUP_DEV, "tp"),
        P(GROUP_DEV, None, "tp"),
        P(GROUP_DEV, None, "tp"),
        P("tp", DEV),
        P("tp", None),
        P(None, DEV),
    )
    return jax.shard_map(
        per_device, mesh=finer, in_specs=placed, out_specs=P("group", DEV), check_vma=False
    )
```
